256 devices in a mesh: freq: 32 (over x, z), pts: 8 (over y, core).
Axes of the slice: x: 4, y: 4, z: 8, core: 2. Of those that a mesh axis runs over, the one named last changes fastest.
Arguments:
- snapshots: float32 [256, 5, 65536], P(None, None, ('pts', 'freq')), may hold values from -6 to 6
- weights: float32 [65536], P(('pts', 'freq')), may hold values from 0.25 to 4
- starts: int32 [3], replicated, may hold values from 0 to 128
- bins: int32 [64], replicated, may hold values from 0 to 63, each once
Outputs:
- modes: float32 [64, 2, 5, 65536], P('freq', None, None, 'pts')
- energy: float32 [64], P('freq')
The draws below stay inside these ranges and needn't reach their ends.
All inputs are finite; a program needn't handle non-finite values.
Results may differ from the reference program's by a relative error of at most 0.00024.
Values sent between devices are 32-bit elements; how exact they have to be, the bound alone decides.
A program may use at most 64 MiB of HBM per device.

```python
import math
import jax
import jax.numpy as jnp
from jax import lax

NVAR = 5
NFFT = 128
NB = 3
ITERS = 8
KF = 64
NT = 256
NPTS = 65536


def block_scale(stream_key, dims, shards, least, largest):
    def one(dim, shards_of):
        steps = jax.random.uniform(jax.random.fold_in(jax.random.fold_in(stream_key, 6), dim), (shards_of,), jnp.float32, least / len(shards), largest / len(shards))
        return jnp.repeat(jnp.exp(steps), dims[dim] // shards_of).reshape((-1,) + (1,) * (len(dims) - dim - 1))

    loudness = one(*shards[0])
    for cut in shards[1:]:
        loudness = loudness * one(*cut)
    return loudness


def noise(stream_key, dims, deviation, limit, shards=(), kind=jnp.bfloat16):
    drawn = jax.random.normal(stream_key, dims, jnp.float32) * deviation
    if len(shards) > 0:
        drawn = block_scale(stream_key, dims, shards, -0.22, 0.18) * drawn
    return jnp.clip(drawn, min=-limit, max=limit).astype(kind)


def setup_inputs(seed: int = 0) -> dict:
    seeds = jax.random.split(jax.random.key(seed), 5)
    return {
        "snapshots": noise(seeds[0], (NT, NVAR, NPTS), 1.0, 6.0, ((2, 256),), jnp.float32),
        "weights": jnp.clip(jnp.exp(math.log(4.0) - 2.7725887 * jax.random.uniform(seeds[1], (NPTS,), jnp.float32) ** block_scale(seeds[1], (NPTS,), ((0, 256),), -0.2, 0.2)), 0.25, 4.0),
        "starts": jax.random.randint(seeds[2], (NB,), 0, NT - NFFT + 1).astype(jnp.int32),
        "bins": jax.random.permutation(seeds[3], KF).astype(jnp.int32),
    }


def dft_window():
    steps_t = jnp.arange(NFFT, dtype=jnp.float32)
    window = 0.5 - 0.5 * jnp.cos(2.0 * math.pi * steps_t / NFFT)
    return (window, 1.0 / jnp.sqrt(jnp.sum(window * window)))

def gram_of(spec, wts, count):
    weighted = spec * wts
    real_part = jnp.einsum('kacvp,kbcvp->kab', weighted, spec, precision=lax.Precision.HIGHEST)
    cross = jnp.einsum('kavp,kbvp->kab', weighted[:, :, 0], spec[:, :, 1], precision=lax.Precision.HIGHEST)
    return (real_part / count, (cross - jnp.swapaxes(cross, 1, 2)) / count)

def apply_gram(gram_re, gram_im, xr, xi):
    ur = lax.optimization_barrier(jnp.sum(gram_re * xr[:, None, :], 2)) - lax.optimization_barrier(jnp.sum(gram_im * xi[:, None, :], 2))
    ui = lax.optimization_barrier(jnp.sum(gram_re * xi[:, None, :], 2)) + lax.optimization_barrier(jnp.sum(gram_im * xr[:, None, :], 2))
    return (ur, ui)

def leading(gram_re, gram_im):
    xr = jnp.ones(gram_re.shape[:2], gram_re.dtype)
    xi = jnp.zeros(gram_re.shape[:2], gram_re.dtype)
    for step in range(ITERS):
        ur, ui = apply_gram(gram_re, gram_im, xr, xi)
        scale_now = jnp.sqrt(lax.optimization_barrier(jnp.sum(ur * ur + ui * ui, 1)))[:, None]
        xr, xi = (ur / scale_now, ui / scale_now)
    ur, ui = apply_gram(gram_re, gram_im, xr, xi)
    return (xr, xi, lax.optimization_barrier(jnp.sum(xr * ur + xi * ui, 1)))

def build_modes(spec, xr, xi, energy):
    hp = lax.Precision.HIGHEST
    real_part = jnp.einsum('kb,kbvp->kvp', xr, spec[:, :, 0], precision=hp) - jnp.einsum('kb,kbvp->kvp', xi, spec[:, :, 1], precision=hp)
    imag_part = jnp.einsum('kb,kbvp->kvp', xr, spec[:, :, 1], precision=hp) + jnp.einsum('kb,kbvp->kvp', xi, spec[:, :, 0], precision=hp)
    factor = 1.0 / jnp.sqrt(jnp.maximum(energy, 0.25))
    return jnp.stack([real_part, imag_part], 1) * factor[:, None, None, None]

def reference(snapshots, weights, starts, bins):
    centered = snapshots - lax.optimization_barrier(jnp.mean(snapshots, 0, keepdims=True))
    window, scale = dft_window()
    blocks = []
    for block in range(NB):
        segment = lax.dynamic_slice_in_dim(centered, starts[block].astype(jnp.int32), NFFT, 0)
        transformed = jnp.fft.rfft(segment * window[:, None, None], axis=0)[bins.astype(jnp.int32)]
        blocks.append(jnp.stack([jnp.real(transformed), jnp.imag(transformed)], 1) * scale)
    spec = jnp.stack(blocks, 1)
    gram_re, gram_im = gram_of(spec, weights, NPTS * NVAR)
    xr, xi, energy = leading(gram_re, gram_im)
    return (build_modes(spec, xr, xi, energy), energy)
```

```python
import functools
import math

import jax
import jax.numpy as jnp
from jax import lax
from jax.experimental import pallas as pl
from jax.experimental.pallas import tpu as pltpu
from jax.sharding import PartitionSpec as P

NFFT = 128
NB = 3
ITERS = 8
HALF = 64
PAIRS = ((0, 1), (0, 2), (1, 2))
MESH = pl.DeviceIdType.MESH


def half_angle(steps):
    h = steps.astype(jnp.float32) * (math.pi / NFFT)
    z = h * h
    s = jnp.float32(1.0 / math.factorial(13))
    for n in (11, 9, 7, 5, 3, 1):
        s = (1.0 if (n // 2) % 2 == 0 else -1.0) / math.factorial(n) + s * z
    c = jnp.float32(1.0 / math.factorial(12))
    for n in (10, 8, 6, 4, 2, 0):
        c = (1.0 if (n // 2) % 2 == 0 else -1.0) / math.factorial(n) + c * z
    return s * h, c


def split(value):
    high = value.astype(jnp.bfloat16)
    return high, (value - high.astype(jnp.float32)).astype(jnp.bfloat16)


def fill_tables(starts, bins, lhs, kf, n_time):
    shape = (kf, n_time)
    row = jnp.broadcast_to(bins[...].astype(jnp.float32), (kf, kf))
    eye = lax.broadcasted_iota(jnp.int32, (kf, kf), 0) == lax.broadcasted_iota(
        jnp.int32, (kf, kf), 1
    )
    column = jnp.sum(jnp.where(eye, row, 0.0), axis=1, keepdims=True).astype(jnp.int32)
    lane = lax.broadcasted_iota(jnp.int32, shape, 1)
    scale = 1.0 / math.sqrt(NFFT * 3 / 8)
    for block in range(NB):
        t = lane - starts[block]
        sin_w, _ = half_angle(jnp.clip(64 - jnp.abs(t - 64), 0, 64))
        window = sin_w * sin_w * scale
        window = jnp.where((t >= 0) & (t < NFFT), window, 0.0)
        sin_h, cos_h = half_angle((((column * t) + 64) & (NFFT - 1)) - 64)
        for part, table in enumerate((1.0 - 2.0 * sin_h * sin_h, -2.0 * sin_h * cos_h)):
            rows = pl.ds((2 * block + part) * kf, kf)
            high, low = split(table * window)
            lhs[rows, 0:n_time] = high
            lhs[rows, n_time : 2 * n_time] = high
            lhs[rows, 2 * n_time : 3 * n_time] = low


def eight_bins(spec, kf, octet, v, cut):
    return [
        [spec[v, pl.ds((2 * b + part) * kf + octet * 8, 8), cut] for part in range(2)]
        for b in range(NB)
    ]


def exchange(value, mine, axis, length, source, landed, sends, recvs):
    me = lax.axis_index(axis)
    source[...] = value
    landed[me] = value

    def copy(peer, slot):
        return pltpu.make_async_remote_copy(
            src_ref=source,
            dst_ref=landed.at[slot],
            send_sem=sends.at[peer],
            recv_sem=recvs.at[slot],
            device_id={axis: peer},
            device_id_type=MESH,
        )

    def send(d, carry):
        copy(lax.rem(me + length - d, length), me).start()
        return carry

    def wait(d, carry):
        peer = lax.rem(me + d, length)
        copy(peer, peer).wait_recv()
        return carry

    def drain(d, carry):
        copy(lax.rem(me + length - d, length), me).wait_send()
        return carry

    lax.fori_loop(1, length, send, 0)
    lax.fori_loop(1, length, wait, 0)
    total = landed[0]
    for peer in range(1, length):
        total += landed[peer]
    return total, lambda: lax.fori_loop(1, length, drain, 0)


def leading(total):
    other = pltpu.roll(total, HALF, 1)
    q = [(total if n % 2 == 0 else other)[n // 2 : n // 2 + 1, :] for n in range(9)]
    re = {(a, a): q[a] for a in range(NB)}
    im = {}
    for n, (a, c) in enumerate(PAIRS):
        re[a, c] = re[c, a] = q[3 + n]
        im[a, c], im[c, a] = q[6 + n], -q[6 + n]

    def apply(xr, xi):
        ur, ui = [], []
        for a in range(NB):
            r, i = re[a, a] * xr[a], re[a, a] * xi[a]
            for c in range(NB):
                if c != a:
                    r = r + (re[a, c] * xr[c] - im[a, c] * xi[c])
                    i = i + (re[a, c] * xi[c] + im[a, c] * xr[c])
            ur.append(r)
            ui.append(i)
        return ur, ui

    def step(_, x):
        ur, ui = apply(x[:NB], x[NB:])
        norm = sum(r * r + i * i for r, i in zip(ur, ui))
        scale = 1.0 / jnp.sqrt(norm)
        return tuple(r * scale for r in ur) + tuple(i * scale for i in ui)

    one = jnp.ones_like(q[0])
    x = lax.fori_loop(0, ITERS, step, (one,) * NB + (one - one,) * NB)
    ur, ui = apply(x[:NB], x[NB:])
    energy = sum(x[a] * ur[a] + x[NB + a] * ui[a] for a in range(NB))
    factor = 1.0 / jnp.sqrt(jnp.maximum(energy, 0.25))
    return [v * factor for v in x], energy


def kernel(
    sizes, snap, wts, starts, bins, rec, energy_out,
    xbuf, lhs, rhs, spec, acc, g1, g1r, g2, g2r, coef, send,
    load_sem, s1, r1, s2, r2, s3, r3,
):
    n_freq, n_pts, kf, n_var, n_time, n_local = sizes
    per_dev = kf // n_freq
    me_f, me_p = lax.axis_index("freq"), lax.axis_index("pts")

    def load(v):
        return pltpu.make_async_copy(snap.at[v], xbuf.at[v], load_sem.at[v])

    for v in range(n_var):
        load(v).start()

    barrier = pltpu.get_barrier_semaphore()

    def greet(axis, me, length):
        def one(d, carry):
            pl.semaphore_signal(
                barrier,
                inc=1,
                device_id={axis: lax.rem(me + d, length)},
                device_id_type=MESH,
            )
            return carry

        lax.fori_loop(1, length, one, 0)

    greet("freq", me_f, n_freq)
    greet("pts", me_p, n_pts)

    fill_tables(starts, bins, lhs, kf, n_time)
    acc[...] = jnp.zeros_like(acc)

    def transform(v, carry):
        load(v).wait()
        x = xbuf[v]
        x = x - jnp.sum(x, axis=0, keepdims=True) * (1.0 / n_time)
        high, low = split(x)
        rhs[0:n_time, :] = high
        rhs[n_time : 2 * n_time, :] = low
        rhs[2 * n_time : 3 * n_time, :] = high
        spec[v] = jnp.dot(lhs[...], rhs[...], preferred_element_type=jnp.float32)
        return carry

    lax.fori_loop(0, n_var, transform, 0)

    cuts = [slice(128 * n, 128 * n + 128) for n in range(n_local // 128)]

    def gram(octet, carry):
        sums = [jnp.zeros((8, 128), jnp.float32)] * 9
        for v in range(n_var):
            for cut in cuts:
                s = eight_bins(spec, kf, octet, v, cut)
                w = jnp.broadcast_to(wts[:, cut], (8, 128))
                ws = [[w * part for part in one] for one in s]
                terms = [ws[a][0] * s[a][0] + ws[a][1] * s[a][1] for a in range(NB)]
                terms += [ws[a][0] * s[c][0] + ws[a][1] * s[c][1] for a, c in PAIRS]
                terms += [ws[a][0] * s[c][1] - ws[a][1] * s[c][0] for a, c in PAIRS]
                sums = [x + y for x, y in zip(sums, terms)]
        for n in range(9):
            acc[pl.ds(n * HALF + octet * 8, 8), :] = sums[n]
        return carry

    lax.fori_loop(0, kf // 8, gram, 0)

    parts = acc[...]
    first = parts.astype(jnp.bfloat16)
    second, third = split(parts - first.astype(jnp.float32))
    by_lane = lax.dot_general(
        jnp.ones((8, 3 * 128), jnp.bfloat16),
        jnp.concatenate([first, second, third], axis=1),
        (((1,), (1,)), ((), ())),
        preferred_element_type=jnp.float32,
    )
    sublane = lax.broadcasted_iota(jnp.int32, (8, 128), 0)
    mine = jnp.zeros((8, 128), jnp.float32)
    for n in range(5):
        mine = jnp.where(sublane == n, by_lane[:, n * 128 : n * 128 + 128], mine)

    pl.semaphore_wait(barrier, n_freq + n_pts - 2)
    near, drain_near = exchange(mine, me_p, "pts", n_pts, g1, g1r, s1, r1)
    total, drain_far = exchange(near, me_f, "freq", n_freq, g2, g2r, s2, r2)
    total = total / float(n_freq * n_pts * n_local * n_var)

    coefs, energy = leading(total)
    energy_out[...] = pltpu.roll(energy, lax.rem(128 - per_dev * me_f, 128), 1)
    table = jnp.zeros((128, 128), jnp.float32)
    wide = lax.broadcasted_iota(jnp.int32, (128, 128), 0)
    for n, c in enumerate(coefs):
        table = jnp.where(wide == n, jnp.broadcast_to(c, (128, 128)), table)
    coef[...] = jnp.transpose(table)

    dests = 8 // per_dev
    rows = per_dev * n_var * 2 * len(cuts)
    stride = rows // per_dev

    def give(dest, slot):
        return pltpu.make_async_remote_copy(
            src_ref=send.at[pl.ds(dest * rows, rows), :],
            dst_ref=rec.at[pl.ds(slot * rows, rows), :],
            send_sem=s3.at[dest],
            recv_sem=r3.at[slot],
            device_id={"freq": dest},
            device_id_type=MESH,
        )

    n_oct = kf // 8

    def modes(i, carry):
        octet = lax.rem(me_f // dests + 1 + i, n_oct)
        c = coef[pl.ds(octet * 8, 8), :]
        wide = [jnp.broadcast_to(c[:, n : n + 1], (8, 128)) for n in range(2 * NB)]
        for v in range(n_var):
            for n, cut in enumerate(cuts):
                s = eight_bins(spec, kf, octet, v, cut)
                re = sum(wide[b] * s[b][0] - wide[NB + b] * s[b][1] for b in range(NB))
                im = sum(wide[b] * s[b][1] + wide[NB + b] * s[b][0] for b in range(NB))
                for part, value in enumerate((re, im)):
                    at = octet * (8 * stride) + (v * len(cuts) + n) * 2 + part
                    send[pl.ds(at, 8, stride=stride), :] = value
        for d in range(dests):
            dest = octet * dests + d

            @pl.when(dest != me_f)
            def _():
                give(dest, me_f).start()

            @pl.when(dest == me_f)
            def _():
                rec[pl.ds(me_f * rows, rows), :] = send[pl.ds(me_f * rows, rows), :]

        return carry

    lax.fori_loop(0, n_oct, modes, 0)

    def take(d, carry):
        peer = lax.rem(me_f + d, n_freq)
        give(peer, peer).wait_recv()
        return carry

    def sent(d, carry):
        give(lax.rem(me_f + d, n_freq), me_f).wait_send()
        return carry

    lax.fori_loop(1, n_freq, take, 0)
    lax.fori_loop(1, n_freq, sent, 0)
    drain_near()
    drain_far()


def body(n_freq, n_pts, snapshots, weights, starts, bins):
    n_time, n_var, n_local = snapshots.shape
    kf = bins.shape[0]
    per_dev = kf // n_freq
    tiles = n_local // 128
    rows = kf * n_var * 2 * tiles
    sizes = (n_freq, n_pts, kf, n_var, n_time, n_local)
    vmem = pl.BlockSpec(memory_space=pltpu.VMEM)
    dma = pltpu.SemaphoreType.DMA
    rec, energy = pl.pallas_call(
        functools.partial(kernel, sizes),
        out_shape=(
            jax.ShapeDtypeStruct((rows, 128), jnp.float32),
            jax.ShapeDtypeStruct((1, 128), jnp.float32),
        ),
        in_specs=[
            pl.BlockSpec(memory_space=pl.ANY),
            vmem,
            pl.BlockSpec(memory_space=pltpu.SMEM),
            vmem,
        ],
        out_specs=(vmem, vmem),
        scratch_shapes=[
            pltpu.VMEM((n_var, n_time, n_local), jnp.float32),
            pltpu.VMEM((2 * NB * kf, 3 * n_time), jnp.bfloat16),
            pltpu.VMEM((3 * n_time, n_local), jnp.bfloat16),
            pltpu.VMEM((n_var, 2 * NB * kf, n_local), jnp.float32),
            pltpu.VMEM((10 * HALF, 128), jnp.float32),
            pltpu.VMEM((8, 128), jnp.float32),
            pltpu.VMEM((n_pts, 8, 128), jnp.float32),
            pltpu.VMEM((8, 128), jnp.float32),
            pltpu.VMEM((n_freq, 8, 128), jnp.float32),
            pltpu.VMEM((128, 128), jnp.float32),
            pltpu.VMEM((rows, 128), jnp.float32),
            dma((n_var,)),
            dma((n_pts,)),
            dma((n_pts,)),
            dma((n_freq,)),
            dma((n_freq,)),
            dma((n_freq,)),
            dma((n_freq,)),
        ],
        compiler_params=pltpu.CompilerParams(collective_id=0, has_side_effects=True),
    )(jnp.transpose(snapshots, (1, 0, 2)), weights.reshape(1, -1), starts, bins.reshape(1, -1))
    modes = rec.reshape(n_freq, per_dev, n_var, tiles, 2, 128)
    modes = jnp.transpose(modes, (1, 4, 2, 0, 3, 5)).reshape(
        per_dev, 2, n_var, n_freq * n_local
    )
    return modes, energy[0, :per_dev]


def solution(mesh):
    n_freq, n_pts = mesh.shape["freq"], mesh.shape["pts"]
    return jax.shard_map(
        functools.partial(body, n_freq, n_pts),
        mesh=mesh,
        in_specs=(P(None, None, ("pts", "freq")), P(("pts", "freq")), P(), P()),
        out_specs=(P("freq", None, None, "pts"), P("freq")),
        check_vma=False,
    )
```

```python
import functools
import math

import jax
import jax.numpy as jnp
from jax import lax
from jax.experimental import pallas as pl
from jax.experimental.pallas import tpu as pltpu
from jax.sharding import PartitionSpec as P

NFFT = 128
NB = 3
ITERS = 8
HALF = 64
PAIRS = ((0, 1), (0, 2), (1, 2))
MESH = pl.DeviceIdType.MESH


def half_angle(steps):
    h = steps.astype(jnp.float32) * (math.pi / NFFT)
    z = h * h
    s = jnp.float32(1.0 / math.factorial(13))
    for n in (11, 9, 7, 5, 3, 1):
        s = (1.0 if (n // 2) % 2 == 0 else -1.0) / math.factorial(n) + s * z
    c = jnp.float32(1.0 / math.factorial(12))
    for n in (10, 8, 6, 4, 2, 0):
        c = (1.0 if (n // 2) % 2 == 0 else -1.0) / math.factorial(n) + c * z
    return s * h, c


def split(value):
    high = value.astype(jnp.bfloat16)
    return high, (value - high.astype(jnp.float32)).astype(jnp.bfloat16)


def fill_tables(starts, bins, lhs, kf, n_time):
    shape = (kf, n_time)
    row = jnp.broadcast_to(bins[...].astype(jnp.float32), (kf, kf))
    eye = lax.broadcasted_iota(jnp.int32, (kf, kf), 0) == lax.broadcasted_iota(
        jnp.int32, (kf, kf), 1
    )
    column = jnp.sum(jnp.where(eye, row, 0.0), axis=1, keepdims=True).astype(jnp.int32)
    lane = lax.broadcasted_iota(jnp.int32, shape, 1)
    scale = 1.0 / math.sqrt(NFFT * 3 / 8)
    for block in range(NB):
        t = lane - starts[block]
        sin_w, _ = half_angle(jnp.clip(64 - jnp.abs(t - 64), 0, 64))
        window = sin_w * sin_w * scale
        window = jnp.where((t >= 0) & (t < NFFT), window, 0.0)
        sin_h, cos_h = half_angle((((column * t) + 64) & (NFFT - 1)) - 64)
        for part, table in enumerate((1.0 - 2.0 * sin_h * sin_h, -2.0 * sin_h * cos_h)):
            rows = pl.ds((2 * block + part) * kf, kf)
            high, low = split(table * window)
            lhs[rows, 0:n_time] = high
            lhs[rows, n_time : 2 * n_time] = high
            lhs[rows, 2 * n_time : 3 * n_time] = low


def eight_bins(spec, kf, octet, v, cut):
    return [
        [spec[v, pl.ds((2 * b + part) * kf + octet * 8, 8), cut] for part in range(2)]
        for b in range(NB)
    ]


def exchange(value, mine, axis, length, source, landed, sends, recvs):
    me = lax.axis_index(axis)
    source[...] = value
    landed[me] = value

    def copy(peer, slot):
        return pltpu.make_async_remote_copy(
            src_ref=source,
            dst_ref=landed.at[slot],
            send_sem=sends.at[peer],
            recv_sem=recvs.at[slot],
            device_id={axis: peer},
            device_id_type=MESH,
        )

    def send(d, carry):
        copy(lax.rem(me + length - d, length), me).start()
        return carry

    def wait(d, carry):
        peer = lax.rem(me + d, length)
        copy(peer, peer).wait_recv()
        return carry

    def drain(d, carry):
        copy(lax.rem(me + length - d, length), me).wait_send()
        return carry

    lax.fori_loop(1, length, send, 0)
    lax.fori_loop(1, length, wait, 0)
    total = landed[0]
    for peer in range(1, length):
        total += landed[peer]
    return total, lambda: lax.fori_loop(1, length, drain, 0)


def leading(total):
    other = pltpu.roll(total, HALF, 1)
    q = [(total if n % 2 == 0 else other)[n // 2 : n // 2 + 1, :] for n in range(9)]
    re = {(a, a): q[a] for a in range(NB)}
    im = {}
    for n, (a, c) in enumerate(PAIRS):
        re[a, c] = re[c, a] = q[3 + n]
        im[a, c], im[c, a] = q[6 + n], -q[6 + n]

    def apply(xr, xi):
        ur, ui = [], []
        for a in range(NB):
            r, i = re[a, a] * xr[a], re[a, a] * xi[a]
            for c in range(NB):
                if c != a:
                    r = r + (re[a, c] * xr[c] - im[a, c] * xi[c])
                    i = i + (re[a, c] * xi[c] + im[a, c] * xr[c])
            ur.append(r)
            ui.append(i)
        return ur, ui

    def step(_, x):
        ur, ui = apply(x[:NB], x[NB:])
        norm = sum(r * r + i * i for r, i in zip(ur, ui))
        scale = 1.0 / jnp.sqrt(norm)
        return tuple(r * scale for r in ur) + tuple(i * scale for i in ui)

    one = jnp.ones_like(q[0])
    x = lax.fori_loop(0, ITERS, step, (one,) * NB + (one - one,) * NB)
    ur, ui = apply(x[:NB], x[NB:])
    energy = sum(x[a] * ur[a] + x[NB + a] * ui[a] for a in range(NB))
    factor = 1.0 / jnp.sqrt(jnp.maximum(energy, 0.25))
    return [v * factor for v in x], energy


def kernel(
    sizes, snap, wts, starts, bins, rec, energy_out,
    xbuf, lhs, rhs, spec, acc, g1, g1r, g2, g2r, coef, send,
    load_sem, s1, r1, s2, r2, s3, r3,
):
    n_freq, n_pts, kf, n_var, n_time, n_local = sizes
    per_dev = kf // n_freq
    me_f, me_p = lax.axis_index("freq"), lax.axis_index("pts")

    def load(v):
        return pltpu.make_async_copy(snap.at[v], xbuf.at[v], load_sem.at[v])

    for v in range(n_var):
        load(v).start()

    barrier = pltpu.get_barrier_semaphore()

    def greet(axis, me, length):
        def one(d, carry):
            pl.semaphore_signal(
                barrier,
                inc=1,
                device_id={axis: lax.rem(me + d, length)},
                device_id_type=MESH,
            )
            return carry

        lax.fori_loop(1, length, one, 0)

    greet("freq", me_f, n_freq)
    greet("pts", me_p, n_pts)

    fill_tables(starts, bins, lhs, kf, n_time)
    acc[...] = jnp.zeros_like(acc)

    def transform(v, carry):
        load(v).wait()
        x = xbuf[v]
        x = x - jnp.sum(x, axis=0, keepdims=True) * (1.0 / n_time)
        high, low = split(x)
        rhs[0:n_time, :] = high
        rhs[n_time : 2 * n_time, :] = low
        rhs[2 * n_time : 3 * n_time, :] = high
        spec[v] = jnp.dot(lhs[...], rhs[...], preferred_element_type=jnp.float32)
        return carry

    lax.fori_loop(0, n_var, transform, 0)

    cuts = [slice(128 * n, 128 * n + 128) for n in range(n_local // 128)]

    def gram(octet, carry):
        sums = [jnp.zeros((8, 128), jnp.float32)] * 9
        for v in range(n_var):
            for cut in cuts:
                s = eight_bins(spec, kf, octet, v, cut)
                w = jnp.broadcast_to(wts[:, cut], (8, 128))
                ws = [[w * part for part in one] for one in s]
                terms = [ws[a][0] * s[a][0] + ws[a][1] * s[a][1] for a in range(NB)]
                terms += [ws[a][0] * s[c][0] + ws[a][1] * s[c][1] for a, c in PAIRS]
                terms += [ws[a][0] * s[c][1] - ws[a][1] * s[c][0] for a, c in PAIRS]
                sums = [x + y for x, y in zip(sums, terms)]
        for n in range(9):
            acc[pl.ds(n * HALF + octet * 8, 8), :] = sums[n]
        return carry

    lax.fori_loop(0, kf // 8, gram, 0)

    parts = acc[...]
    first = parts.astype(jnp.bfloat16)
    second, third = split(parts - first.astype(jnp.float32))
    by_lane = lax.dot_general(
        jnp.ones((8, 3 * 128), jnp.bfloat16),
        jnp.concatenate([first, second, third], axis=1),
        (((1,), (1,)), ((), ())),
        preferred_element_type=jnp.float32,
    )
    sublane = lax.broadcasted_iota(jnp.int32, (8, 128), 0)
    mine = jnp.zeros((8, 128), jnp.float32)
    for n in range(5):
        mine = jnp.where(sublane == n, by_lane[:, n * 128 : n * 128 + 128], mine)

    pl.semaphore_wait(barrier, n_freq + n_pts - 2)
    near, drain_near = exchange(mine, me_p, "pts", n_pts, g1, g1r, s1, r1)
    total, drain_far = exchange(near, me_f, "freq", n_freq, g2, g2r, s2, r2)
    total = total / float(n_freq * n_pts * n_local * n_var)

    coefs, energy = leading(total)
    energy_out[...] = pltpu.roll(energy, lax.rem(128 - per_dev * me_f, 128), 1)
    table = jnp.zeros((128, 128), jnp.float32)
    wide = lax.broadcasted_iota(jnp.int32, (128, 128), 0)
    for n, c in enumerate(coefs):
        table = jnp.where(wide == n, jnp.broadcast_to(c, (128, 128)), table)
    coef[...] = jnp.transpose(table)

    dests = 8 // per_dev
    rows = per_dev * n_var * 2 * len(cuts)
    stride = rows // per_dev

    def give(dest, slot):
        return pltpu.make_async_remote_copy(
            src_ref=send.at[pl.ds(dest * rows, rows), :],
            dst_ref=rec.at[pl.ds(slot * rows, rows), :],
            send_sem=s3.at[dest],
            recv_sem=r3.at[slot],
            device_id={"freq": dest},
            device_id_type=MESH,
        )

    n_oct = kf // 8

    def modes(i, carry):
        octet = lax.rem(me_f // dests + 1 + i, n_oct)
        c = coef[pl.ds(octet * 8, 8), :]
        wide = [jnp.broadcast_to(c[:, n : n + 1], (8, 128)) for n in range(2 * NB)]
        for v in range(n_var):
            for n, cut in enumerate(cuts):
                s = eight_bins(spec, kf, octet, v, cut)
                re = sum(wide[b] * s[b][0] - wide[NB + b] * s[b][1] for b in range(NB))
                im = sum(wide[b] * s[b][1] + wide[NB + b] * s[b][0] for b in range(NB))
                for part, value in enumerate((re, im)):
                    at = octet * (8 * stride) + (v * len(cuts) + n) * 2 + part
                    send[pl.ds(at, 8, stride=stride), :] = value
        for d in range(dests):
            dest = octet * dests + d

            @pl.when(dest != me_f)
            def _():
                give(dest, me_f).start()

            @pl.when(dest == me_f)
            def _():
                rec[pl.ds(me_f * rows, rows), :] = send[pl.ds(me_f * rows, rows), :]

        return carry

    lax.fori_loop(0, n_oct, modes, 0)

    def take(d, carry):
        peer = lax.rem(me_f + d, n_freq)
        give(peer, peer).wait_recv()
        return carry

    def sent(d, carry):
        give(lax.rem(me_f + d, n_freq), me_f).wait_send()
        return carry

    lax.fori_loop(1, n_freq, take, 0)
    lax.fori_loop(1, n_freq, sent, 0)
    drain_near()
    drain_far()


def body(n_freq, n_pts, snapshots, weights, starts, bins):
    n_time, n_var, n_local = snapshots.shape
    kf = bins.shape[0]
    per_dev = kf // n_freq
    tiles = n_local // 128
    rows = kf * n_var * 2 * tiles
    sizes = (n_freq, n_pts, kf, n_var, n_time, n_local)
    vmem = pl.BlockSpec(memory_space=pltpu.VMEM)
    dma = pltpu.SemaphoreType.DMA
    rec, energy = pl.pallas_call(
        functools.partial(kernel, sizes),
        out_shape=(
            jax.ShapeDtypeStruct((rows, 128), jnp.float32),
            jax.ShapeDtypeStruct((1, 128), jnp.float32),
        ),
        in_specs=[
            pl.BlockSpec(memory_space=pl.ANY),
            vmem,
            pl.BlockSpec(memory_space=pltpu.SMEM),
            vmem,
        ],
        out_specs=(vmem, vmem),
        scratch_shapes=[
            pltpu.VMEM((n_var, n_time, n_local), jnp.float32),
            pltpu.VMEM((2 * NB * kf, 3 * n_time), jnp.bfloat16),
            pltpu.VMEM((3 * n_time, n_local), jnp.bfloat16),
            pltpu.VMEM((n_var, 2 * NB * kf, n_local), jnp.float32),
            pltpu.VMEM((10 * HALF, 128), jnp.float32),
            pltpu.VMEM((8, 128), jnp.float32),
            pltpu.VMEM((n_pts, 8, 128), jnp.float32),
            pltpu.VMEM((8, 128), jnp.float32),
            pltpu.VMEM((n_freq, 8, 128), jnp.float32),
            pltpu.VMEM((128, 128), jnp.float32),
            pltpu.VMEM((rows, 128), jnp.float32),
            dma((n_var,)),
            dma((n_pts,)),
            dma((n_pts,)),
            dma((n_freq,)),
            dma((n_freq,)),
            dma((n_freq,)),
            dma((n_freq,)),
        ],
        compiler_params=pltpu.CompilerParams(collective_id=0, has_side_effects=True),
    )(jnp.transpose(snapshots, (1, 0, 2)), weights.reshape(1, -1), starts, bins.reshape(1, -1))
    modes = rec.reshape(n_freq, per_dev * n_var, 2 * tiles, 128)
    modes = jnp.transpose(modes, (1, 0, 2, 3)).reshape(per_dev, n_var, n_freq * tiles, 2, 128)
    modes = jnp.transpose(modes, (0, 3, 1, 2, 4)).reshape(per_dev, 2, n_var, n_freq * n_local)
    return modes, energy[0, :per_dev]


def solution(mesh):
    n_freq, n_pts = mesh.shape["freq"], mesh.shape["pts"]
    return jax.shard_map(
        functools.partial(body, n_freq, n_pts),
        mesh=mesh,
        in_specs=(P(None, None, ("pts", "freq")), P(("pts", "freq")), P(), P()),
        out_specs=(P("freq", None, None, "pts"), P("freq")),
        check_vma=False,
    )
```

```python
import functools
import math

import jax
import jax.numpy as jnp
from jax import lax
from jax.experimental import pallas as pl
from jax.experimental.pallas import tpu as pltpu
from jax.sharding import PartitionSpec as P

NFFT = 128
NB = 3
ITERS = 8
HALF = 64
PAIRS = ((0, 1), (0, 2), (1, 2))
MESH = pl.DeviceIdType.MESH


def half_angle(steps):
    h = steps.astype(jnp.float32) * (math.pi / NFFT)
    z = h * h
    s = jnp.float32(1.0 / math.factorial(13))
    for n in (11, 9, 7, 5, 3, 1):
        s = (1.0 if (n // 2) % 2 == 0 else -1.0) / math.factorial(n) + s * z
    c = jnp.float32(1.0 / math.factorial(12))
    for n in (10, 8, 6, 4, 2, 0):
        c = (1.0 if (n // 2) % 2 == 0 else -1.0) / math.factorial(n) + c * z
    return s * h, c


def split(value):
    high = value.astype(jnp.bfloat16)
    return high, (value - high.astype(jnp.float32)).astype(jnp.bfloat16)


def fill_tables(starts, bins, lhs, kf, n_time):
    shape = (kf, n_time)
    row = jnp.broadcast_to(bins[...].astype(jnp.float32), (kf, kf))
    eye = lax.broadcasted_iota(jnp.int32, (kf, kf), 0) == lax.broadcasted_iota(
        jnp.int32, (kf, kf), 1
    )
    column = jnp.sum(jnp.where(eye, row, 0.0), axis=1, keepdims=True).astype(jnp.int32)
    lane = lax.broadcasted_iota(jnp.int32, shape, 1)
    scale = 1.0 / math.sqrt(NFFT * 3 / 8)
    for block in range(NB):
        t = lane - starts[block]
        sin_w, _ = half_angle(jnp.clip(64 - jnp.abs(t - 64), 0, 64))
        window = sin_w * sin_w * scale
        window = jnp.where((t >= 0) & (t < NFFT), window, 0.0)
        sin_h, cos_h = half_angle((((column * t) + 64) & (NFFT - 1)) - 64)
        for part, table in enumerate((1.0 - 2.0 * sin_h * sin_h, -2.0 * sin_h * cos_h)):
            rows = pl.ds((2 * block + part) * kf, kf)
            high, low = split(table * window)
            lhs[rows, 0:n_time] = high
            lhs[rows, n_time : 2 * n_time] = high
            lhs[rows, 2 * n_time : 3 * n_time] = low


def eight_bins(spec, kf, octet, v, cut):
    return [
        [spec[v, pl.ds((2 * b + part) * kf + octet * 8, 8), cut] for part in range(2)]
        for b in range(NB)
    ]


def exchange(value, slot, group, source, landed, sent, came):
    source[...] = value
    landed[slot] = value
    for peer in group:
        pltpu.make_async_remote_copy(
            src_ref=source,
            dst_ref=landed.at[slot],
            send_sem=sent,
            recv_sem=came,
            device_id=peer,
            device_id_type=MESH,
        ).start()
    held = landed.at[pl.ds(0, len(group))]
    pltpu.make_async_copy(held, held, came).wait()
    total = landed[0]
    for n in range(1, len(group) + 1):
        total += landed[n]
    return total, lambda: pltpu.make_async_copy(held, held, sent).wait()


def groups_of(sizes):
    nx, nz, ny = sizes
    f, p = lax.axis_index("freq"), lax.axis_index("pts")
    x, z, y, core = f // nz, lax.rem(f, nz), p // 2, lax.rem(p, 2)

    def far(d, n):
        return min(d, n - d)

    steps = [(i, j) for i in range(nx) for j in range(ny) if i or j]
    steps.sort(key=lambda s: -far(s[0], nx) - far(s[1], ny))
    plane = [
        {"freq": lax.rem(x + i, nx) * nz + z, "pts": lax.rem(y + j, ny) * 2 + core}
        for i, j in steps
    ]
    steps = [(i, j) for i in range(nz) for j in range(2) if i or j]
    steps.sort(key=lambda s: -far(s[0], nz) - 0.5 * s[1])
    line = [
        {"freq": x * nz + lax.rem(z + i, nz), "pts": y * 2 + lax.rem(core + j, 2)}
        for i, j in steps
    ]
    return (x * ny + y, plane), (z * 2 + core, line)


def leading(total):
    other = pltpu.roll(total, HALF, 1)
    q = [(total if n % 2 == 0 else other)[n // 2 : n // 2 + 1, :] for n in range(9)]
    re = {(a, a): q[a] for a in range(NB)}
    im = {}
    for n, (a, c) in enumerate(PAIRS):
        re[a, c] = re[c, a] = q[3 + n]
        im[a, c], im[c, a] = q[6 + n], -q[6 + n]

    def apply(xr, xi):
        ur, ui = [], []
        for a in range(NB):
            r, i = re[a, a] * xr[a], re[a, a] * xi[a]
            for c in range(NB):
                if c != a:
                    r = r + (re[a, c] * xr[c] - im[a, c] * xi[c])
                    i = i + (re[a, c] * xi[c] + im[a, c] * xr[c])
            ur.append(r)
            ui.append(i)
        return ur, ui

    def step(_, x):
        ur, ui = apply(x[:NB], x[NB:])
        norm = sum(r * r + i * i for r, i in zip(ur, ui))
        scale = 1.0 / jnp.sqrt(norm)
        return tuple(r * scale for r in ur) + tuple(i * scale for i in ui)

    one = jnp.ones_like(q[0])
    x = lax.fori_loop(0, ITERS, step, (one,) * NB + (one - one,) * NB)
    ur, ui = apply(x[:NB], x[NB:])
    energy = sum(x[a] * ur[a] + x[NB + a] * ui[a] for a in range(NB))
    factor = 1.0 / jnp.sqrt(jnp.maximum(energy, 0.25))
    return [v * factor for v in x], energy


def kernel(
    sizes, split_sizes, snap, wts_in, starts_in, bins_in, rec, energy_out,
    wts, starts, bins, xbuf, lhs, rhs, spec, acc, g1, g1r, g2, g2r, coef, send,
    load_sem, small_sem, s1, r1, s2, r2, s3, r3,
):
    n_freq, n_pts, kf, n_var, n_time, n_local = sizes
    per_dev = kf // n_freq
    me_f = lax.axis_index("freq")

    def load(v):
        return pltpu.make_async_copy(snap.at[v], xbuf.at[v], load_sem.at[v])

    small = [
        pltpu.make_async_copy(source, target, small_sem.at[n])
        for n, (source, target) in enumerate(
            ((bins_in, bins), (starts_in, starts), (wts_in, wts))
        )
    ]
    for copy in small:
        copy.start()
    for v in range(n_var):
        load(v).start()

    barrier = pltpu.get_barrier_semaphore()
    near_group, far_group = groups_of(split_sizes)
    everyone = far_group[1] + near_group[1]
    for peer in everyone:
        pl.semaphore_signal(barrier, inc=1, device_id=peer, device_id_type=MESH)

    acc[...] = jnp.zeros_like(acc)
    for copy in small:
        copy.wait()
    fill_tables(starts, bins, lhs, kf, n_time)

    def transform(v, carry):
        load(v).wait()
        x = xbuf[v]
        x = x - jnp.sum(x, axis=0, keepdims=True) * (1.0 / n_time)
        high, low = split(x)
        rhs[0:n_time, :] = high
        rhs[n_time : 2 * n_time, :] = low
        rhs[2 * n_time : 3 * n_time, :] = high
        spec[v] = jnp.dot(lhs[...], rhs[...], preferred_element_type=jnp.float32)
        return carry

    lax.fori_loop(0, n_var, transform, 0)

    cuts = [slice(128 * n, 128 * n + 128) for n in range(n_local // 128)]

    def gram(octet, carry):
        sums = [jnp.zeros((8, 128), jnp.float32)] * 9
        for v in range(n_var):
            for cut in cuts:
                s = eight_bins(spec, kf, octet, v, cut)
                w = jnp.broadcast_to(wts[:, cut], (8, 128))
                ws = [[w * part for part in one] for one in s]
                terms = [ws[a][0] * s[a][0] + ws[a][1] * s[a][1] for a in range(NB)]
                terms += [ws[a][0] * s[c][0] + ws[a][1] * s[c][1] for a, c in PAIRS]
                terms += [ws[a][0] * s[c][1] - ws[a][1] * s[c][0] for a, c in PAIRS]
                sums = [x + y for x, y in zip(sums, terms)]
        for n in range(9):
            acc[pl.ds(n * HALF + octet * 8, 8), :] = sums[n]
        return carry

    lax.fori_loop(0, kf // 8, gram, 0)

    parts = acc[...]
    first = parts.astype(jnp.bfloat16)
    second, third = split(parts - first.astype(jnp.float32))
    by_lane = lax.dot_general(
        jnp.ones((8, 3 * 128), jnp.bfloat16),
        jnp.concatenate([first, second, third], axis=1),
        (((1,), (1,)), ((), ())),
        preferred_element_type=jnp.float32,
    )
    sublane = lax.broadcasted_iota(jnp.int32, (8, 128), 0)
    mine = jnp.zeros((8, 128), jnp.float32)
    for n in range(5):
        mine = jnp.where(sublane == n, by_lane[:, n * 128 : n * 128 + 128], mine)

    pl.semaphore_wait(barrier, len(everyone))
    near, drain_near = exchange(mine[:5], *near_group, g1, g1r, s1, r1)
    total, drain_far = exchange(near, *far_group, g2, g2r, s2, r2)
    total = total / float(n_freq * n_pts * n_local * n_var)

    coefs, energy = leading(total)
    energy_out[...] = pltpu.roll(energy, lax.rem(128 - per_dev * me_f, 128), 1)
    table = jnp.zeros((128, 128), jnp.float32)
    wide = lax.broadcasted_iota(jnp.int32, (128, 128), 0)
    for n, c in enumerate(coefs):
        table = jnp.where(wide == n, jnp.broadcast_to(c, (128, 128)), table)
    coef[...] = jnp.transpose(table)

    dests = 8 // per_dev
    rows = per_dev * n_var * 2 * len(cuts)
    stride = rows // per_dev

    def give(dest, slot):
        return pltpu.make_async_remote_copy(
            src_ref=send.at[pl.ds(dest * rows, rows), :],
            dst_ref=rec.at[pl.ds(slot * rows, rows), :],
            send_sem=s3,
            recv_sem=r3,
            device_id={"freq": dest},
            device_id_type=MESH,
        )

    n_oct = kf // 8

    def modes(i, carry):
        octet = lax.rem(me_f // dests + 1 + i, n_oct)
        c = coef[pl.ds(octet * 8, 8), :]
        wide = [jnp.broadcast_to(c[:, n : n + 1], (8, 128)) for n in range(2 * NB)]
        for v in range(n_var):
            for n, cut in enumerate(cuts):
                s = eight_bins(spec, kf, octet, v, cut)
                re = sum(wide[b] * s[b][0] - wide[NB + b] * s[b][1] for b in range(NB))
                im = sum(wide[b] * s[b][1] + wide[NB + b] * s[b][0] for b in range(NB))
                for part, value in enumerate((re, im)):
                    at = octet * (8 * stride) + (v * len(cuts) + n) * 2 + part
                    send[pl.ds(at, 8, stride=stride), :] = value
        for d in range(dests):
            dest = octet * dests + d

            @pl.when(dest != me_f)
            def _():
                give(dest, me_f).start()

            @pl.when(dest == me_f)
            def _():
                rec[pl.ds(me_f * rows, rows), :] = send[pl.ds(me_f * rows, rows), :]

        return carry

    lax.fori_loop(0, n_oct, modes, 0)

    others = rec.at[pl.ds(0, (n_freq - 1) * rows), :]
    pltpu.make_async_copy(others, others, r3).wait()
    pltpu.make_async_copy(others, others, s3).wait()
    drain_near()
    drain_far()


def write_out(groups, n_freq, lines, per_dev, rec, row, modes, energy, sems):
    copies = [
        pltpu.make_async_copy(rec.at[:, g], modes.at[g], sems.at[g]) for g in range(groups)
    ]
    for copy in copies:
        copy.start()
    energy[...] = row[0, :per_dev]
    for copy in copies:
        copy.wait()


def body(n_freq, n_pts, nz, snapshots, weights, starts, bins):
    n_time, n_var, n_local = snapshots.shape
    kf = bins.shape[0]
    per_dev = kf // n_freq
    tiles = n_local // 128
    rows = kf * n_var * 2 * tiles
    sizes = (n_freq, n_pts, kf, n_var, n_time, n_local)
    split_sizes = (n_freq // nz, nz, n_pts // 2)
    near, far = split_sizes[0] * split_sizes[2], 2 * nz
    vmem, anywhere = (pl.BlockSpec(memory_space=m) for m in (pltpu.VMEM, pl.ANY))
    dma = pltpu.SemaphoreType.DMA
    rec, energy = pl.pallas_call(
        functools.partial(kernel, sizes, split_sizes),
        out_shape=(
            pltpu.VMEM((rows, 128), jnp.float32),
            pltpu.VMEM((1, 128), jnp.float32),
        ),
        in_specs=[anywhere] * 4,
        out_specs=(vmem, vmem),
        scratch_shapes=[
            pltpu.VMEM((1, n_local), jnp.float32),
            pltpu.SMEM((NB,), jnp.int32),
            pltpu.VMEM((1, kf), jnp.int32),
            pltpu.VMEM((n_var, n_time, n_local), jnp.float32),
            pltpu.VMEM((2 * NB * kf, 3 * n_time), jnp.bfloat16),
            pltpu.VMEM((3 * n_time, n_local), jnp.bfloat16),
            pltpu.VMEM((n_var, 2 * NB * kf, n_local), jnp.float32),
            pltpu.VMEM((10 * HALF, 128), jnp.float32),
            pltpu.VMEM((5, 128), jnp.float32),
            pltpu.VMEM((near, 5, 128), jnp.float32),
            pltpu.VMEM((5, 128), jnp.float32),
            pltpu.VMEM((far, 5, 128), jnp.float32),
            pltpu.VMEM((128, 128), jnp.float32),
            pltpu.VMEM((rows, 128), jnp.float32),
            dma((n_var,)),
            dma((3,)),
        ]
        + [pltpu.SemaphoreType.DMA(())] * 6,
        compiler_params=pltpu.CompilerParams(collective_id=0, has_side_effects=True),
    )(jnp.transpose(snapshots, (1, 0, 2)), weights.reshape(1, -1), starts, bins.reshape(1, -1))
    groups = per_dev * n_var
    modes, energy = pl.pallas_call(
        functools.partial(write_out, groups, n_freq, 2 * tiles, per_dev),
        out_shape=(
            jax.ShapeDtypeStruct((groups, n_freq, 2 * tiles, 128), jnp.float32),
            jax.ShapeDtypeStruct((per_dev,), jnp.float32),
        ),
        in_specs=[vmem, vmem],
        out_specs=(pl.BlockSpec(memory_space=pl.ANY), vmem),
        scratch_shapes=[dma((groups,))],
    )(
        pltpu.with_memory_space_constraint(
            rec.reshape(n_freq, groups, 2 * tiles, 128), pltpu.VMEM
        ),
        pltpu.with_memory_space_constraint(energy, pltpu.VMEM),
    )
    modes = modes.reshape(per_dev, n_var, n_freq * tiles, 2, 128)
    modes = jnp.transpose(modes, (0, 3, 1, 2, 4)).reshape(
        per_dev, 2, n_var, n_freq * n_local
    )
    return modes, energy


def solution(mesh):
    n_freq, n_pts = mesh.shape["freq"], mesh.shape["pts"]
    return jax.shard_map(
        functools.partial(body, n_freq, n_pts, 8 if n_freq % 8 == 0 else 2),
        mesh=mesh,
        in_specs=(P(None, None, ("pts", "freq")), P(("pts", "freq")), P(), P()),
        out_specs=(P("freq", None, None, "pts"), P("freq")),
        check_vma=False,
    )
```

```python
import functools
import math

import jax
import jax.numpy as jnp
from jax import lax
from jax.experimental import pallas as pl
from jax.experimental.pallas import tpu as pltpu
from jax.sharding import PartitionSpec as P

NFFT = 128
NB = 3
ITERS = 8
LENGTH_Z = 8
HALF = 64
PAIRS = ((0, 1), (0, 2), (1, 2))
MESH = pl.DeviceIdType.MESH


def half_angle(steps):
    h = steps.astype(jnp.float32) * (math.pi / NFFT)
    z = h * h
    s = jnp.float32(1.0 / math.factorial(13))
    for n in (11, 9, 7, 5, 3, 1):
        s = (1.0 if (n // 2) % 2 == 0 else -1.0) / math.factorial(n) + s * z
    c = jnp.float32(1.0 / math.factorial(12))
    for n in (10, 8, 6, 4, 2, 0):
        c = (1.0 if (n // 2) % 2 == 0 else -1.0) / math.factorial(n) + c * z
    return s * h, c


def split(value):
    high = value.astype(jnp.bfloat16)
    return high, (value - high.astype(jnp.float32)).astype(jnp.bfloat16)


def fill_tables(starts, bins, lhs, kf, n_time, per_dev):
    n_dev = kf // per_dev
    slot = lax.broadcasted_iota(jnp.int32, (kf, kf), 0)
    slot = lax.rem(slot, n_dev) * per_dev + slot // n_dev
    here = lax.broadcasted_iota(jnp.int32, (kf, kf), 1) == slot
    row = jnp.broadcast_to(bins[...].astype(jnp.float32), (kf, kf))
    column = jnp.sum(jnp.where(here, row, 0.0), axis=1, keepdims=True).astype(jnp.int32)
    lane = lax.broadcasted_iota(jnp.int32, (kf, NFFT), 1)
    time = lax.broadcasted_iota(jnp.int32, (1, n_time), 1)
    scale = 1.0 / math.sqrt(NFFT * 3 / 8)
    for block in range(NB):
        t = time - starts[block]
        sin_w, _ = half_angle(jnp.clip(64 - jnp.abs(t - 64), 0, 64))
        window = sin_w * sin_w * scale
        window = jnp.where((t >= 0) & (t < NFFT), window, 0.0)
        t = lane - starts[block]
        sin_h, cos_h = half_angle((((column * t) + 64) & (NFFT - 1)) - 64)
        for part, table in enumerate((1.0 - 2.0 * sin_h * sin_h, -2.0 * sin_h * cos_h)):
            rows = pl.ds((2 * block + part) * kf, kf)
            for n in range(n_time // NFFT):
                high, low = split(table * window[:, n * NFFT : (n + 1) * NFFT])
                for third, value in enumerate((high, high, low)):
                    at = third * n_time + n * NFFT
                    lhs[rows, at : at + NFFT] = value


def eight_bins(spec, kf, octet, v, cut):
    return [
        [spec[v, pl.ds((2 * b + part) * kf + octet * 8, 8), cut] for part in range(2)]
        for b in range(NB)
    ]


def exchange(slot, group, source, landed, sent, came):
    shared = sum(number == 0 for _, number in group)

    def wait(count, sem):
        held = landed.at[pl.ds(0, count)]
        pltpu.make_async_copy(held, held, sem).wait()

    def start(value):
        source[...] = value
        landed[slot] = value
        for peer, number in group:
            pltpu.make_async_remote_copy(
                src_ref=source,
                dst_ref=landed.at[slot],
                send_sem=sent,
                recv_sem=came.at[number],
                device_id=peer,
                device_id_type=MESH,
            ).start()

    def one(number):
        wait(1, came.at[number])

    def finish():
        wait(shared, came.at[0])
        total = landed[0]
        for n in range(1, len(group) + 1):
            total += landed[n]
        return total

    def drain():
        wait(len(group), sent)

    return start, one, finish, drain


def groups_of(sizes):
    nx, nz, ny = sizes
    f, p = lax.axis_index("freq"), lax.axis_index("pts")
    x, z, y, core = f // nz, lax.rem(f, nz), p // 2, lax.rem(p, 2)

    def far(d, n):
        return min(d, n - d)

    steps = [(i, j) for i in range(nx) for j in range(ny) if i or j]
    steps.sort(key=lambda s: -far(s[0], nx) - far(s[1], ny))
    plane = [
        ({"freq": lax.rem(x + i, nx) * nz + z, "pts": lax.rem(y + j, ny) * 2 + core}, 0 if j else i)
        for i, j in steps
    ]
    steps = [(i, j) for i in range(nz) for j in range(2) if i or j]
    steps.sort(key=lambda s: -far(s[0], nz) - 0.5 * s[1])
    line = [
        ({"freq": x * nz + lax.rem(z + i, nz), "pts": y * 2 + lax.rem(core + j, 2)}, 0)
        for i, j in steps
    ]
    return (x * ny + y, plane), (z * 2 + core, line)


def leading(total):
    other = pltpu.roll(total, HALF, 1)
    q = [(total if n % 2 == 0 else other)[n // 2 : n // 2 + 1, :] for n in range(9)]
    re = {(a, a): q[a] for a in range(NB)}
    im = {}
    for n, (a, c) in enumerate(PAIRS):
        re[a, c] = re[c, a] = q[3 + n]
        im[a, c], im[c, a] = q[6 + n], -q[6 + n]

    def apply(xr, xi):
        ur, ui = [], []
        for a in range(NB):
            r, i = re[a, a] * xr[a], re[a, a] * xi[a]
            for c in range(NB):
                if c != a:
                    r = r + (re[a, c] * xr[c] - im[a, c] * xi[c])
                    i = i + (re[a, c] * xi[c] + im[a, c] * xr[c])
            ur.append(r)
            ui.append(i)
        return ur, ui

    def step(_, x):
        ur, ui = apply(x[:NB], x[NB:])
        norm = sum(r * r + i * i for r, i in zip(ur, ui))
        scale = lax.rsqrt(norm)
        return tuple(r * scale for r in ur) + tuple(i * scale for i in ui)

    one = jnp.ones_like(q[0])
    x = lax.fori_loop(0, ITERS, step, (one,) * NB + (one - one,) * NB)
    ur, ui = apply(x[:NB], x[NB:])
    energy = sum(x[a] * ur[a] + x[NB + a] * ui[a] for a in range(NB))
    factor = 1.0 / jnp.sqrt(jnp.maximum(energy, 0.25))
    return [v * factor for v in x], energy


def kernel(
    sizes, split_sizes, early, snap, wts_in, starts_in, bins_in, rec, tail, energy_out,
    wts, starts, bins, xbuf, lhs, rhs, spec, acc, g1, g1r, g2, g2r, coef, send, ahead, ahead_r,
    load_sem, small_sem, s1, r1, s2, r2, s3, r3, s4, r4,
):
    n_freq, n_pts, kf, n_var, n_time, n_local = sizes
    nx, nz, _ = split_sizes
    per_dev = kf // n_freq
    me_f = lax.axis_index("freq")
    n_oct, wide = n_freq // 8, 8
    cuts = [slice(128 * n, 128 * n + 128) for n in range(n_local // 128)]
    units = [(v, cut) for v in range(n_var) for cut in cuts]
    late, soon = units[: len(units) - early], units[len(units) - early :]

    def load(v):
        return pltpu.make_async_copy(snap.at[v], xbuf.at[v], load_sem.at[v])

    small = [
        pltpu.make_async_copy(source, target, small_sem.at[n])
        for n, (source, target) in enumerate(
            ((bins_in, bins), (starts_in, starts), (wts_in, wts))
        )
    ]
    for copy in small:
        copy.start()
    for v in range(n_var):
        load(v).start()

    barrier = pltpu.get_barrier_semaphore()
    near_group, far_group = groups_of(split_sizes)
    everyone = far_group[1] + near_group[1]
    for peer, _ in everyone:
        pl.semaphore_signal(barrier, inc=1, device_id=peer, device_id_type=MESH)

    acc[...] = jnp.zeros_like(acc)
    for copy in small:
        copy.wait()
    fill_tables(starts, bins, lhs, kf, n_time, per_dev)

    def centre(v, slot):
        x = xbuf[v]
        x = x - jnp.sum(x, axis=0, keepdims=True) * (1.0 / n_time)
        high, low = split(x)
        rhs[slot, 0:n_time, :] = high
        rhs[slot, n_time : 2 * n_time, :] = low
        rhs[slot, 2 * n_time : 3 * n_time, :] = high

    def gram(v):
        ws = [jnp.broadcast_to(wts[:, cut], (8, 128)) for cut in cuts]
        for octet in range(kf // 8):
            sums = [acc[pl.ds(n * HALF + octet * 8, 8), :] for n in range(9)]
            for w, cut in zip(ws, cuts):
                s = eight_bins(spec, kf, octet, v, cut)
                wt = [[w * part for part in one] for one in s]
                terms = [wt[a][0] * s[a][0] + wt[a][1] * s[a][1] for a in range(NB)]
                terms += [wt[a][0] * s[c][0] + wt[a][1] * s[c][1] for a, c in PAIRS]
                terms += [wt[a][0] * s[c][1] - wt[a][1] * s[c][0] for a, c in PAIRS]
                sums = [x + y for x, y in zip(sums, terms)]
            for n in range(9):
                acc[pl.ds(n * HALF + octet * 8, 8), :] = sums[n]

    def transform(v):
        spec[v] = jnp.dot(lhs[...], rhs[v], preferred_element_type=jnp.float32)

    for v in range(n_var):
        load(v).wait()
    centre(0, 0)
    for v in range(n_var):
        transform(v)
        if v + 1 < n_var:
            centre(v + 1, v + 1)
        if v:
            gram(v - 1)
    gram(n_var - 1)

    parts = acc[...]
    first = parts.astype(jnp.bfloat16)
    second, third = split(parts - first.astype(jnp.float32))
    by_lane = lax.dot_general(
        jnp.ones((8, 3 * 128), jnp.bfloat16),
        jnp.concatenate([first, second, third], axis=1),
        (((1,), (1,)), ((), ())),
        preferred_element_type=jnp.float32,
    )
    sublane = lax.broadcasted_iota(jnp.int32, (8, 128), 0)
    mine = jnp.zeros((8, 128), jnp.float32)
    for n in range(5):
        mine = jnp.where(sublane == n, by_lane[:, n * 128 : n * 128 + 128], mine)

    start_near, one_near, finish_near, drain_near = exchange(*near_group, g1, g1r, s1, r1)
    start_far, _, finish_far, drain_far = exchange(*far_group, g2, g2r, s2, r2)

    pitch = per_dev * early * 2 * NB

    def lead(dest, slot):
        return pltpu.make_async_remote_copy(
            src_ref=ahead.at[pl.ds(dest * pitch, pitch), :],
            dst_ref=ahead_r.at[pl.ds(slot * pitch, pitch), :],
            send_sem=s4,
            recv_sem=r4,
            device_id={"freq": dest},
            device_id_type=MESH,
        )

    def pack(octet, carry):
        for kk in range(per_dev):
            for n, (v, cut) in enumerate(soon):
                s = eight_bins(spec, kf, kk * n_oct + octet, v, cut)
                for b in range(NB):
                    for part in range(2):
                        at = octet * (8 * pitch) + ((kk * early + n) * NB + b) * 2 + part
                        ahead[pl.ds(at, wide, stride=pitch), :] = s[b][part]
        return carry

    if early:
        lax.fori_loop(0, n_oct, pack, 0)
        mine_rows = pl.ds(me_f * pitch, pitch)
        ahead_r[mine_rows, :] = ahead[mine_rows, :]

    x, z = me_f // nz, lax.rem(me_f, nz)

    def send_ahead(dx):
        for dz in range(nz):
            if dx or dz:
                dest = lax.rem(x + dx, nx) * nz + lax.rem(z + dz, nz)
                lead(dest, me_f).start()

    pl.semaphore_wait(barrier, len(everyone))
    start_near(mine[:5])
    send_ahead(0)
    order = sorted(range(1, nx), key=lambda d: min(d, nx - d))
    for n, dx in enumerate(order):
        one_near(nx - dx)
        if n < 1:
            send_ahead(dx)
    near = finish_near()
    start_far(near)
    for dx in order[1:]:
        send_ahead(dx)
    total = finish_far()
    total = total / float(n_freq * n_pts * n_local * n_var)

    coefs, energy = leading(total)
    lane = lax.broadcasted_iota(jnp.int32, (1, 128), 1)
    for kk in range(per_dev):
        turned = pltpu.roll(energy, lax.rem(256 + kk - kk * n_freq - me_f, 128), 1)
        row = turned if kk == 0 else jnp.where(lane == kk, turned, row)
    energy_out[...] = row
    table = jnp.zeros((128, 128), jnp.float32)
    high = lax.broadcasted_iota(jnp.int32, (128, 128), 0)
    for n, c in enumerate(coefs):
        table = jnp.where(high == n, jnp.broadcast_to(c, (128, 128)), table)
    coef[...] = jnp.transpose(table)

    part_rows = len(late) * 2
    rows = per_dev * part_rows
    slot_rows = rows + 8

    def give(dest, slot):
        return pltpu.make_async_remote_copy(
            src_ref=send.at[pl.ds(dest * slot_rows, rows), :],
            dst_ref=rec.at[pl.ds(slot * rows, rows), :],
            send_sem=s3,
            recv_sem=r3,
            device_id={"freq": dest},
            device_id_type=MESH,
        )

    def spread(c):
        return [jnp.broadcast_to(c[:, n : n + 1], (8, 128)) for n in range(2 * NB)]

    def combine(c, s):
        re = sum(c[b] * s[b][0] - c[NB + b] * s[b][1] for b in range(NB))
        im = sum(c[b] * s[b][1] + c[NB + b] * s[b][0] for b in range(NB))
        return re, im

    def modes(i, carry):
        octet = lax.rem(me_f // 8 + 1 + i, n_oct)
        for kk in range(per_dev):
            c = spread(coef[pl.ds(kk * n_freq + octet * 8, 8), :])
            for n, (v, cut) in enumerate(late):
                s = eight_bins(spec, kf, kk * n_oct + octet, v, cut)
                for part, value in enumerate(combine(c, s)):
                    at = octet * (8 * slot_rows) + kk * part_rows + 2 * n + part
                    send[pl.ds(at, wide, stride=slot_rows), :] = value
        for d in range(wide):
            dest = octet * 8 + d

            @pl.when(dest != me_f)
            def _():
                give(dest, me_f).start()

            @pl.when(dest == me_f)
            def _():
                rec[pl.ds(me_f * rows, rows), :] = send[pl.ds(me_f * slot_rows, rows), :]

        return carry

    lax.fori_loop(0, n_oct, modes, 0)

    if early:
        theirs = ahead_r.at[pl.ds(0, (n_freq - 1) * pitch), :]
        pltpu.make_async_copy(theirs, theirs, r4).wait()
        for kk in range(per_dev):
            c = coef[pl.ds(kk * n_freq + me_f, 1), :]
            c = spread(jnp.broadcast_to(c, (8, 128)))
            for octet in range(n_oct):
                for n in range(early):
                    s = [
                        [
                            ahead_r[
                                pl.ds(
                                    octet * 8 * pitch + ((kk * early + n) * NB + b) * 2 + part,
                                    wide,
                                    stride=pitch,
                                ),
                                :,
                            ]
                            for part in range(2)
                        ]
                        for b in range(NB)
                    ]
                    for part, value in enumerate(combine([q for q in c], s)):
                        at = octet * 16 * per_dev * early + (kk * early + n) * 2 + part
                        tail[pl.ds(at, wide, stride=2 * per_dev * early), :] = value

    others = rec.at[pl.ds(0, (n_freq - 1) * rows), :]
    pltpu.make_async_copy(others, others, r3).wait()
    pltpu.make_async_copy(others, others, s3).wait()
    if early:
        pltpu.make_async_copy(theirs, theirs, s4).wait()
    drain_near()
    drain_far()


def write_out(sizes, early, rec, tail, row, modes, energy, sems):
    per_dev, n_var, tiles = sizes
    left = n_var * tiles - early
    copies = []

    def add(source, target):
        copies.append(pltpu.make_async_copy(source, target, sems.at[len(copies)]))

    for kk in range(per_dev):
        for v in range(n_var):
            held = modes.at[kk * n_var + v]
            if (v + 1) * tiles <= left:
                add(rec.at[:, kk, pl.ds(v * tiles, tiles)], held)
            elif v * tiles >= left:
                add(tail.at[:, pl.ds(kk * early + v * tiles - left, tiles)], held)
            else:
                cut = left - v * tiles
                add(rec.at[:, kk, pl.ds(v * tiles, cut)], held.at[:, pl.ds(0, cut)])
                add(
                    tail.at[:, pl.ds(kk * early, tiles - cut)],
                    held.at[:, pl.ds(cut, tiles - cut)],
                )
    for copy in copies:
        copy.start()
    energy[...] = row[0, :per_dev]
    for copy in copies:
        copy.wait()


def body(n_freq, n_pts, nz, snapshots, weights, starts, bins):
    n_time, n_var, n_local = snapshots.shape
    kf = bins.shape[0]
    per_dev = kf // n_freq
    tiles = n_local // 128
    early = 2
    rows = kf * (n_var * tiles - early) * 2
    ahead = max(kf * early * 2 * NB, 8)
    tail_rows = max(kf * early * 2, n_freq * 2)
    sizes = (n_freq, n_pts, kf, n_var, n_time, n_local)
    split_sizes = (n_freq // nz, nz, n_pts // 2)
    near, far = split_sizes[0] * split_sizes[2], 2 * nz
    vmem, anywhere = (pl.BlockSpec(memory_space=m) for m in (pltpu.VMEM, pl.ANY))
    dma = pltpu.SemaphoreType.DMA
    rec, tail, energy = pl.pallas_call(
        functools.partial(kernel, sizes, split_sizes, early),
        out_shape=(
            pltpu.VMEM((rows, 128), jnp.float32),
            pltpu.VMEM((tail_rows, 128), jnp.float32),
            pltpu.VMEM((1, 128), jnp.float32),
        ),
        in_specs=[anywhere] * 4,
        out_specs=(vmem, vmem, vmem),
        scratch_shapes=[
            pltpu.VMEM((1, n_local), jnp.float32),
            pltpu.SMEM((NB,), jnp.int32),
            pltpu.VMEM((1, kf), jnp.int32),
            pltpu.VMEM((n_var, n_time, n_local), jnp.float32),
            pltpu.VMEM((2 * NB * kf, 3 * n_time), jnp.bfloat16),
            pltpu.VMEM((n_var, 3 * n_time, n_local), jnp.bfloat16),
            pltpu.VMEM((n_var, 2 * NB * kf, n_local), jnp.float32),
            pltpu.VMEM((10 * HALF, 128), jnp.float32),
            pltpu.VMEM((5, 128), jnp.float32),
            pltpu.VMEM((near, 5, 128), jnp.float32),
            pltpu.VMEM((5, 128), jnp.float32),
            pltpu.VMEM((far, 5, 128), jnp.float32),
            pltpu.VMEM((128, 128), jnp.float32),
            pltpu.VMEM((rows + 8 * n_freq, 128), jnp.float32),
            pltpu.VMEM((ahead, 128), jnp.float32),
            pltpu.VMEM((ahead, 128), jnp.float32),
            dma((n_var,)),
            dma((3,)),
        ]
        + [dma(()), dma((split_sizes[0],)), dma(()), dma((1,))]
        + [dma(())] * 4,
        compiler_params=pltpu.CompilerParams(collective_id=0, has_side_effects=True),
    )(jnp.transpose(snapshots, (1, 0, 2)), weights.reshape(1, -1), starts, bins.reshape(1, -1))
    held = [
        pltpu.with_memory_space_constraint(value, pltpu.VMEM)
        for value in (
            rec.reshape(n_freq, per_dev, -1, 2, 128),
            tail.reshape(n_freq, -1, 2, 128),
            energy,
        )
    ]
    modes, energy = pl.pallas_call(
        functools.partial(write_out, (per_dev, n_var, tiles), early),
        out_shape=(
            jax.ShapeDtypeStruct((per_dev * n_var, n_freq, tiles, 2, 128), jnp.float32),
            jax.ShapeDtypeStruct((per_dev,), jnp.float32),
        ),
        in_specs=[vmem] * 3,
        out_specs=(anywhere, vmem),
        scratch_shapes=[dma((2 * per_dev * n_var,))],
    )(*held)
    modes = modes.reshape(per_dev, n_var, n_freq * tiles, 2, 128)
    modes = jnp.transpose(modes, (0, 3, 1, 2, 4)).reshape(
        per_dev, 2, n_var, n_freq * n_local
    )
    return modes, energy


def solution(mesh):
    n_freq, n_pts = mesh.shape["freq"], mesh.shape["pts"]
    return jax.shard_map(
        functools.partial(body, n_freq, n_pts, LENGTH_Z),
        mesh=mesh,
        in_specs=(P(None, None, ("pts", "freq")), P(("pts", "freq")), P(), P()),
        out_specs=(P("freq", None, None, "pts"), P("freq")),
        check_vma=False,
    )
```

```python
import functools
import itertools
import math

import jax
import jax.numpy as jnp
from jax import lax
from jax.experimental import pallas as pl
from jax.experimental.pallas import tpu as pltpu
from jax.sharding import PartitionSpec as P

NFFT = 128
NB = 3
ITERS = 8
LENGTH_Z = 8
FAR_FIRST = (4, 3, 5, 2, 6, 1, 7, 0)
HALF = 64
PAIRS = ((0, 1), (0, 2), (1, 2))
MESH = pl.DeviceIdType.MESH


def half_angle(steps):
    h = steps.astype(jnp.float32) * (math.pi / NFFT)
    z = h * h
    s = jnp.float32(1.0 / math.factorial(13))
    for n in (11, 9, 7, 5, 3, 1):
        s = (1.0 if (n // 2) % 2 == 0 else -1.0) / math.factorial(n) + s * z
    c = jnp.float32(1.0 / math.factorial(12))
    for n in (10, 8, 6, 4, 2, 0):
        c = (1.0 if (n // 2) % 2 == 0 else -1.0) / math.factorial(n) + c * z
    return s * h, c


def split(value):
    high = value.astype(jnp.bfloat16)
    return high, (value - high.astype(jnp.float32)).astype(jnp.bfloat16)


def fill_tables(starts, bins, lhs, kf, n_time, per_dev):
    n_dev = kf // per_dev
    slot = lax.broadcasted_iota(jnp.int32, (kf, kf), 0)
    slot = lax.rem(slot, n_dev) * per_dev + slot // n_dev
    here = lax.broadcasted_iota(jnp.int32, (kf, kf), 1) == slot
    row = jnp.broadcast_to(bins[...].astype(jnp.float32), (kf, kf))
    column = jnp.sum(jnp.where(here, row, 0.0), axis=1, keepdims=True).astype(jnp.int32)
    lane = lax.broadcasted_iota(jnp.int32, (kf, NFFT), 1)
    time = lax.broadcasted_iota(jnp.int32, (1, n_time), 1)
    scale = 1.0 / math.sqrt(NFFT * 3 / 8)
    for block in range(NB):
        t = time - starts[block]
        sin_w, _ = half_angle(jnp.clip(64 - jnp.abs(t - 64), 0, 64))
        window = sin_w * sin_w * scale
        window = jnp.where((t >= 0) & (t < NFFT), window, 0.0)
        t = lane - starts[block]
        sin_h, cos_h = half_angle((((column * t) + 64) & (NFFT - 1)) - 64)
        for part, table in enumerate((1.0 - 2.0 * sin_h * sin_h, -2.0 * sin_h * cos_h)):
            rows = pl.ds((2 * block + part) * kf, kf)
            for n in range(n_time // NFFT):
                high, low = split(table * window[:, n * NFFT : (n + 1) * NFFT])
                for third, value in enumerate((high, high, low)):
                    at = third * n_time + n * NFFT
                    lhs[rows, at : at + NFFT] = value


def eight_bins(spec, kf, octet, v, cut):
    return [
        [spec[v, pl.ds((2 * b + part) * kf + octet * 8, 8), cut] for part in range(2)]
        for b in range(NB)
    ]


def exchange(slot, group, source, landed, sent, came):
    shared = sum(number == 0 for _, number in group)

    def wait(count, sem):
        held = landed.at[pl.ds(0, count)]
        pltpu.make_async_copy(held, held, sem).wait()

    def start(value):
        source[...] = value
        landed[slot] = value
        for peer, number in group:
            pltpu.make_async_remote_copy(
                src_ref=source,
                dst_ref=landed.at[slot],
                send_sem=sent,
                recv_sem=came.at[number],
                device_id=peer,
                device_id_type=MESH,
            ).start()

    def one(number):
        wait(1, came.at[number])

    def finish():
        wait(shared, came.at[0])
        total = landed[0]
        for n in range(1, len(group) + 1):
            total += landed[n]
        return total

    def drain():
        wait(len(group), sent)

    return start, one, finish, drain


def groups_of(sizes):
    nx, nz, ny = sizes
    f, p = lax.axis_index("freq"), lax.axis_index("pts")
    x, z, y, core = f // nz, lax.rem(f, nz), p // 2, lax.rem(p, 2)

    def far(d, n):
        return min(d, n - d)

    steps = [(i, j) for i in range(nx) for j in range(ny) if i or j]
    steps.sort(key=lambda s: -far(s[0], nx) - far(s[1], ny))
    plane = [
        ({"freq": lax.rem(x + i, nx) * nz + z, "pts": lax.rem(y + j, ny) * 2 + core}, 0)
        for i, j in steps
    ]
    steps = [(i, j) for i in range(nz) for j in range(2) if i or j]
    steps.sort(key=lambda s: -far(s[0], nz) - 0.5 * s[1])
    line = [
        ({"freq": x * nz + lax.rem(z + i, nz), "pts": y * 2 + lax.rem(core + j, 2)}, 0 if j else i)
        for i, j in steps
    ]
    return (z * 2 + core, line), (x * ny + y, plane)


def leading(total):
    other = pltpu.roll(total, HALF, 1)
    q = [(total if n % 2 == 0 else other)[n // 2 : n // 2 + 1, :] for n in range(9)]
    re = {(a, a): q[a] for a in range(NB)}
    im = {}
    for n, (a, c) in enumerate(PAIRS):
        re[a, c] = re[c, a] = q[3 + n]
        im[a, c], im[c, a] = q[6 + n], -q[6 + n]

    def apply(xr, xi):
        ur, ui = [], []
        for a in range(NB):
            r, i = re[a, a] * xr[a], re[a, a] * xi[a]
            for c in range(NB):
                if c != a:
                    r = r + (re[a, c] * xr[c] - im[a, c] * xi[c])
                    i = i + (re[a, c] * xi[c] + im[a, c] * xr[c])
            ur.append(r)
            ui.append(i)
        return ur, ui

    def step(_, x):
        ur, ui = apply(x[:NB], x[NB:])
        norm = sum(r * r + i * i for r, i in zip(ur, ui))
        scale = lax.rsqrt(norm)
        return tuple(r * scale for r in ur) + tuple(i * scale for i in ui)

    one = jnp.ones_like(q[0])
    x = lax.fori_loop(0, ITERS, step, (one,) * NB + (one - one,) * NB)
    ur, ui = apply(x[:NB], x[NB:])
    energy = sum(x[a] * ur[a] + x[NB + a] * ui[a] for a in range(NB))
    factor = 1.0 / jnp.sqrt(jnp.maximum(energy, 0.25))
    return [v * factor for v in x], energy


def kernel(
    sizes, split_sizes, early, snap, wts_in, starts_in, bins_in, rec, tail, energy_out,
    wts, starts, bins, xbuf, lhs, rhs, spec, acc, g1, g1r, g2, g2r, coef, send, ahead, ahead_r,
    load_sem, small_sem, s1, r1, s2, r2, s3, r3, s4, r4,
):
    n_freq, n_pts, kf, n_var, n_time, n_local = sizes
    nx, nz, _ = split_sizes
    per_dev = kf // n_freq
    me_f = lax.axis_index("freq")
    n_oct, wide = n_freq // 8, 8
    cuts = [slice(128 * n, 128 * n + 128) for n in range(n_local // 128)]
    units = [(v, cut) for v in range(n_var) for cut in cuts]
    late, soon = units[: len(units) - early], units[len(units) - early :]

    def load(v):
        return pltpu.make_async_copy(snap.at[v], xbuf.at[v], load_sem.at[v])

    small = [
        pltpu.make_async_copy(source, target, small_sem.at[n])
        for n, (source, target) in enumerate(
            ((bins_in, bins), (starts_in, starts), (wts_in, wts))
        )
    ]
    for copy in small:
        copy.start()
    for v in range(n_var):
        load(v).start()

    barrier = pltpu.get_barrier_semaphore()
    near_group, far_group = groups_of(split_sizes)
    everyone = [p for pair in itertools.zip_longest(far_group[1], near_group[1]) for p in pair if p]
    for peer, _ in everyone:
        pl.semaphore_signal(barrier, inc=1, device_id=peer, device_id_type=MESH)

    acc[...] = jnp.zeros_like(acc)
    for copy in small:
        copy.wait()
    fill_tables(starts, bins, lhs, kf, n_time, per_dev)

    def centre(v, slot):
        x = xbuf[v]
        x = x - jnp.sum(x, axis=0, keepdims=True) * (1.0 / n_time)
        high, low = split(x)
        rhs[slot, 0:n_time, :] = high
        rhs[slot, n_time : 2 * n_time, :] = low
        rhs[slot, 2 * n_time : 3 * n_time, :] = high

    def gram(v):
        ws = [jnp.broadcast_to(wts[:, cut], (8, 128)) for cut in cuts]
        for octet in range(kf // 8):
            sums = [acc[pl.ds(n * HALF + octet * 8, 8), :] for n in range(9)]
            for w, cut in zip(ws, cuts):
                s = eight_bins(spec, kf, octet, v, cut)
                wt = [[w * part for part in one] for one in s]
                terms = [wt[a][0] * s[a][0] + wt[a][1] * s[a][1] for a in range(NB)]
                terms += [wt[a][0] * s[c][0] + wt[a][1] * s[c][1] for a, c in PAIRS]
                terms += [wt[a][0] * s[c][1] - wt[a][1] * s[c][0] for a, c in PAIRS]
                sums = [x + y for x, y in zip(sums, terms)]
            for n in range(9):
                acc[pl.ds(n * HALF + octet * 8, 8), :] = sums[n]

    def transform(v):
        spec[v] = jnp.dot(lhs[...], rhs[v], preferred_element_type=jnp.float32)

    for v in range(n_var):
        load(v).wait()
    centre(0, 0)
    for v in range(n_var):
        transform(v)
        if v + 1 < n_var:
            centre(v + 1, v + 1)
        if v:
            gram(v - 1)
    gram(n_var - 1)

    parts = acc[...]
    first = parts.astype(jnp.bfloat16)
    second, third = split(parts - first.astype(jnp.float32))
    by_lane = lax.dot_general(
        jnp.ones((8, 3 * 128), jnp.bfloat16),
        jnp.concatenate([first, second, third], axis=1),
        (((1,), (1,)), ((), ())),
        preferred_element_type=jnp.float32,
    )
    sublane = lax.broadcasted_iota(jnp.int32, (8, 128), 0)
    mine = jnp.zeros((8, 128), jnp.float32)
    for n in range(5):
        mine = jnp.where(sublane == n, by_lane[:, n * 128 : n * 128 + 128], mine)

    start_near, one_near, finish_near, drain_near = exchange(*near_group, g1, g1r, s1, r1)
    start_far, _, finish_far, drain_far = exchange(*far_group, g2, g2r, s2, r2)

    pitch = per_dev * early * 2 * NB

    def lead(dest, slot):
        return pltpu.make_async_remote_copy(
            src_ref=ahead.at[pl.ds(dest * pitch, pitch), :],
            dst_ref=ahead_r.at[pl.ds(slot * pitch, pitch), :],
            send_sem=s4,
            recv_sem=r4,
            device_id={"freq": dest},
            device_id_type=MESH,
        )

    def pack(octet, carry):
        for kk in range(per_dev):
            for n, (v, cut) in enumerate(soon):
                s = eight_bins(spec, kf, kk * n_oct + octet, v, cut)
                for b in range(NB):
                    for part in range(2):
                        at = octet * (8 * pitch) + ((kk * early + n) * NB + b) * 2 + part
                        ahead[pl.ds(at, wide, stride=pitch), :] = s[b][part]
        return carry

    if early:
        lax.fori_loop(0, n_oct, pack, 0)
        mine_rows = pl.ds(me_f * pitch, pitch)
        ahead_r[mine_rows, :] = ahead[mine_rows, :]

    x, z = me_f // nz, lax.rem(me_f, nz)

    def send_ahead(dz, steps):
        for dx in steps:
            dest = lax.rem(x + dx, nx) * nz + lax.rem(z + dz, nz)
            lead(dest, me_f).start()

    pl.semaphore_wait(barrier, len(everyone))
    start_near(mine[:5])
    order = sorted(range(1, nz), key=lambda d: min(d, nz - d))
    for dz in reversed(order):
        send_ahead(dz, (0,))
    others = range(1, nx)
    for dz in order[:4]:
        one_near(nz - dz)
        send_ahead(dz, others)
    for dz in order[4:]:
        one_near(nz - dz)
    near = finish_near()
    start_far(near)
    for dz in reversed(order[4:]):
        send_ahead(dz, others)
    send_ahead(0, others)
    total = finish_far()
    total = total / float(n_freq * n_pts * n_local * n_var)

    coefs, energy = leading(total)
    lane = lax.broadcasted_iota(jnp.int32, (1, 128), 1)
    for kk in range(per_dev):
        turned = pltpu.roll(energy, lax.rem(256 + kk - kk * n_freq - me_f, 128), 1)
        row = turned if kk == 0 else jnp.where(lane == kk, turned, row)
    energy_out[...] = row
    table = jnp.zeros((128, 128), jnp.float32)
    high = lax.broadcasted_iota(jnp.int32, (128, 128), 0)
    for n, c in enumerate(coefs):
        table = jnp.where(high == n, jnp.broadcast_to(c, (128, 128)), table)
    coef[...] = jnp.transpose(table)

    part_rows = len(late) * 2
    rows = per_dev * part_rows
    slot_rows = rows + 8

    def give(dest, slot):
        return pltpu.make_async_remote_copy(
            src_ref=send.at[pl.ds(dest * slot_rows, rows), :],
            dst_ref=rec.at[pl.ds(slot * rows, rows), :],
            send_sem=s3,
            recv_sem=r3,
            device_id={"freq": dest},
            device_id_type=MESH,
        )

    def spread(c):
        return [jnp.broadcast_to(c[:, n : n + 1], (8, 128)) for n in range(2 * NB)]

    def combine(c, s):
        re = sum(c[b] * s[b][0] - c[NB + b] * s[b][1] for b in range(NB))
        im = sum(c[b] * s[b][1] + c[NB + b] * s[b][0] for b in range(NB))
        return re, im

    def modes(i, carry):
        octet = lax.rem(me_f // 8 + 1 + i, n_oct)
        for kk in range(per_dev):
            c = spread(coef[pl.ds(kk * n_freq + octet * 8, 8), :])
            for n, (v, cut) in enumerate(late):
                s = eight_bins(spec, kf, kk * n_oct + octet, v, cut)
                for part, value in enumerate(combine(c, s)):
                    at = octet * (8 * slot_rows) + kk * part_rows + 2 * n + part
                    send[pl.ds(at, wide, stride=slot_rows), :] = value
        for d in range(wide):
            dest = octet * 8 + d

            @pl.when(dest != me_f)
            def _():
                give(dest, me_f).start()

            @pl.when(dest == me_f)
            def _():
                rec[pl.ds(me_f * rows, rows), :] = send[pl.ds(me_f * slot_rows, rows), :]

        return carry

    lax.fori_loop(0, n_oct, modes, 0)

    if early:
        theirs = ahead_r.at[pl.ds(0, (n_freq - 1) * pitch), :]
        pltpu.make_async_copy(theirs, theirs, r4).wait()
        for kk in range(per_dev):
            c = coef[pl.ds(kk * n_freq + me_f, 1), :]
            c = spread(jnp.broadcast_to(c, (8, 128)))
            for octet in range(n_oct):
                for n in range(early):
                    s = [
                        [
                            ahead_r[
                                pl.ds(
                                    octet * 8 * pitch + ((kk * early + n) * NB + b) * 2 + part,
                                    wide,
                                    stride=pitch,
                                ),
                                :,
                            ]
                            for part in range(2)
                        ]
                        for b in range(NB)
                    ]
                    for part, value in enumerate(combine([q for q in c], s)):
                        at = octet * 16 * per_dev * early + (kk * early + n) * 2 + part
                        tail[pl.ds(at, wide, stride=2 * per_dev * early), :] = value

    others = rec.at[pl.ds(0, (n_freq - 1) * rows), :]
    pltpu.make_async_copy(others, others, r3).wait()
    pltpu.make_async_copy(others, others, s3).wait()
    if early:
        pltpu.make_async_copy(theirs, theirs, s4).wait()
    drain_near()
    drain_far()


def write_out(sizes, early, rec, tail, row, modes, energy, held_energy, sems, sem):
    per_dev, n_var, tiles = sizes
    left = n_var * tiles - early
    copies = []

    def add(source, target):
        copies.append(pltpu.make_async_copy(source, target, sems.at[len(copies)]))

    for kk in range(per_dev):
        for v in range(n_var):
            held = modes.at[kk * n_var + v]
            if (v + 1) * tiles <= left:
                add(rec.at[:, kk, pl.ds(v * tiles, tiles)], held)
            elif v * tiles >= left:
                add(tail.at[:, pl.ds(kk * early + v * tiles - left, tiles)], held)
            else:
                cut = left - v * tiles
                add(rec.at[:, kk, pl.ds(v * tiles, cut)], held.at[:, pl.ds(0, cut)])
                add(
                    tail.at[:, pl.ds(kk * early, tiles - cut)],
                    held.at[:, pl.ds(cut, tiles - cut)],
                )
    held_energy[...] = row[0, :per_dev]
    last = pltpu.make_async_copy(held_energy, energy, sem)
    last.start()
    for copy in copies:
        copy.start()
    for copy in copies:
        copy.wait()
    last.wait()


def body(n_freq, n_pts, nz, snapshots, weights, starts, bins):
    n_time, n_var, n_local = snapshots.shape
    kf = bins.shape[0]
    per_dev = kf // n_freq
    tiles = n_local // 128
    early = 2
    rows = kf * (n_var * tiles - early) * 2
    ahead = max(kf * early * 2 * NB, 8)
    tail_rows = max(kf * early * 2, n_freq * 2)
    sizes = (n_freq, n_pts, kf, n_var, n_time, n_local)
    split_sizes = (n_freq // nz, nz, n_pts // 2)
    near, far = 2 * nz, split_sizes[0] * split_sizes[2]
    vmem, anywhere = (pl.BlockSpec(memory_space=m) for m in (pltpu.VMEM, pl.ANY))
    dma = pltpu.SemaphoreType.DMA
    rec, tail, energy = pl.pallas_call(
        functools.partial(kernel, sizes, split_sizes, early),
        out_shape=(
            pltpu.VMEM((rows, 128), jnp.float32),
            pltpu.VMEM((tail_rows, 128), jnp.float32),
            pltpu.VMEM((1, 128), jnp.float32),
        ),
        in_specs=[anywhere] * 4,
        out_specs=(vmem, vmem, vmem),
        scratch_shapes=[
            pltpu.VMEM((1, n_local), jnp.float32),
            pltpu.SMEM((NB,), jnp.int32),
            pltpu.VMEM((1, kf), jnp.int32),
            pltpu.VMEM((n_var, n_time, n_local), jnp.float32),
            pltpu.VMEM((2 * NB * kf, 3 * n_time), jnp.bfloat16),
            pltpu.VMEM((n_var, 3 * n_time, n_local), jnp.bfloat16),
            pltpu.VMEM((n_var, 2 * NB * kf, n_local), jnp.float32),
            pltpu.VMEM((10 * HALF, 128), jnp.float32),
            pltpu.VMEM((5, 128), jnp.float32),
            pltpu.VMEM((near, 5, 128), jnp.float32),
            pltpu.VMEM((5, 128), jnp.float32),
            pltpu.VMEM((far, 5, 128), jnp.float32),
            pltpu.VMEM((128, 128), jnp.float32),
            pltpu.VMEM((rows + 8 * n_freq, 128), jnp.float32),
            pltpu.VMEM((ahead, 128), jnp.float32),
            pltpu.VMEM((ahead, 128), jnp.float32),
            dma((n_var,)),
            dma((3,)),
        ]
        + [dma(()), dma((nz,)), dma(()), dma((1,))]
        + [dma(())] * 4,
        compiler_params=pltpu.CompilerParams(collective_id=0, has_side_effects=True),
    )(jnp.transpose(snapshots, (1, 0, 2)), weights.reshape(1, -1), starts, bins.reshape(1, -1))
    held = [
        pltpu.with_memory_space_constraint(value, pltpu.VMEM)
        for value in (
            rec.reshape(n_freq, per_dev, -1, 2, 128),
            tail.reshape(n_freq, -1, 2, 128),
            energy,
        )
    ]
    modes, energy = pl.pallas_call(
        functools.partial(write_out, (per_dev, n_var, tiles), early),
        out_shape=(
            jax.ShapeDtypeStruct((per_dev * n_var, n_freq, tiles, 2, 128), jnp.float32),
            jax.ShapeDtypeStruct((per_dev,), jnp.float32),
        ),
        in_specs=[vmem] * 3,
        out_specs=(anywhere, anywhere),
        scratch_shapes=[
            pltpu.VMEM((per_dev,), jnp.float32),
            dma((2 * per_dev * n_var,)),
            dma(()),
        ],
    )(*held)
    modes = modes.reshape(per_dev, n_var, n_freq * tiles, 2, 128)
    modes = jnp.transpose(modes, (0, 3, 1, 2, 4)).reshape(
        per_dev, 2, n_var, n_freq * n_local
    )
    return modes, energy


def solution(mesh):
    n_freq, n_pts = mesh.shape["freq"], mesh.shape["pts"]
    return jax.shard_map(
        functools.partial(body, n_freq, n_pts, LENGTH_Z),
        mesh=mesh,
        in_specs=(P(None, None, ("pts", "freq")), P(("pts", "freq")), P(), P()),
        out_specs=(P("freq", None, None, "pts"), P("freq")),
        check_vma=False,
    )
```

```python
import functools
import itertools
import math

import jax
import jax.numpy as jnp
from jax import lax
from jax.experimental import pallas as pl
from jax.experimental.pallas import tpu as pltpu
from jax.sharding import PartitionSpec as P

NFFT = 128
NB = 3
ITERS = 8
LENGTH_Z = 8
FAR_FIRST = (4, 3, 5, 2, 6, 1, 7, 0)
HALF = 64
PAIRS = ((0, 1), (0, 2), (1, 2))
MESH = pl.DeviceIdType.MESH


def half_angle(steps):
    h = steps.astype(jnp.float32) * (math.pi / NFFT)
    z = h * h
    s = jnp.float32(1.0 / math.factorial(13))
    for n in (11, 9, 7, 5, 3, 1):
        s = (1.0 if (n // 2) % 2 == 0 else -1.0) / math.factorial(n) + s * z
    c = jnp.float32(1.0 / math.factorial(12))
    for n in (10, 8, 6, 4, 2, 0):
        c = (1.0 if (n // 2) % 2 == 0 else -1.0) / math.factorial(n) + c * z
    return s * h, c


def split(value):
    high = value.astype(jnp.bfloat16)
    return high, (value - high.astype(jnp.float32)).astype(jnp.bfloat16)


def fill_tables(starts, bins, lhs, kf, n_time, per_dev):
    n_dev = kf // per_dev
    slot = lax.broadcasted_iota(jnp.int32, (kf, kf), 0)
    slot = lax.rem(slot, n_dev) * per_dev + slot // n_dev
    here = lax.broadcasted_iota(jnp.int32, (kf, kf), 1) == slot
    row = jnp.broadcast_to(bins[...].astype(jnp.float32), (kf, kf))
    column = jnp.sum(jnp.where(here, row, 0.0), axis=1, keepdims=True).astype(jnp.int32)
    lane = lax.broadcasted_iota(jnp.int32, (kf, NFFT), 1)
    time = lax.broadcasted_iota(jnp.int32, (1, n_time), 1)
    scale = 1.0 / math.sqrt(NFFT * 3 / 8)
    for block in range(NB):
        t = time - starts[block]
        sin_w, _ = half_angle(jnp.clip(64 - jnp.abs(t - 64), 0, 64))
        window = sin_w * sin_w * scale
        window = jnp.where((t >= 0) & (t < NFFT), window, 0.0)
        t = lane - starts[block]
        sin_h, cos_h = half_angle((((column * t) + 64) & (NFFT - 1)) - 64)
        for part, table in enumerate((1.0 - 2.0 * sin_h * sin_h, -2.0 * sin_h * cos_h)):
            rows = pl.ds((2 * block + part) * kf, kf)
            for n in range(n_time // NFFT):
                high, low = split(table * window[:, n * NFFT : (n + 1) * NFFT])
                for third, value in enumerate((high, high, low)):
                    at = third * n_time + n * NFFT
                    lhs[rows, at : at + NFFT] = value


def eight_bins(spec, kf, octet, v, cut):
    return [
        [spec[v, pl.ds((2 * b + part) * kf + octet * 8, 8), cut] for part in range(2)]
        for b in range(NB)
    ]


def exchange(slot, group, source, landed, sent, came):
    shared = sum(number == 0 for _, number in group)

    def wait(count, sem):
        held = landed.at[pl.ds(0, count)]
        pltpu.make_async_copy(held, held, sem).wait()

    def start(value):
        source[...] = value
        landed[slot] = value
        for peer, number in group:
            pltpu.make_async_remote_copy(
                src_ref=source,
                dst_ref=landed.at[slot],
                send_sem=sent,
                recv_sem=came.at[number],
                device_id=peer,
                device_id_type=MESH,
            ).start()

    def one(number):
        wait(1, came.at[number])

    def finish():
        wait(shared, came.at[0])
        total = landed[0]
        for n in range(1, len(group) + 1):
            total += landed[n]
        return total

    def drain():
        wait(len(group), sent)

    return start, one, finish, drain


def groups_of(sizes):
    nx, nz, ny = sizes
    f, p = lax.axis_index("freq"), lax.axis_index("pts")
    x, z, y, core = f // nz, lax.rem(f, nz), p // 2, lax.rem(p, 2)

    def far(d, n):
        return min(d, n - d)

    steps = [(i, j) for i in range(nx) for j in range(ny) if i or j]
    steps.sort(key=lambda s: -far(s[0], nx) - far(s[1], ny))
    plane = [
        ({"freq": lax.rem(x + i, nx) * nz + z, "pts": lax.rem(y + j, ny) * 2 + core}, 0)
        for i, j in steps
    ]
    steps = [(i, j) for i in range(nz) for j in range(2) if i or j]
    steps.sort(key=lambda s: -far(s[0], nz) - 0.5 * s[1])
    line = [
        ({"freq": x * nz + lax.rem(z + i, nz), "pts": y * 2 + lax.rem(core + j, 2)}, 0 if j else i)
        for i, j in steps
    ]
    return (z * 2 + core, line), (x * ny + y, plane)


def leading(total):
    other = pltpu.roll(total, HALF, 1)
    q = [(total if n % 2 == 0 else other)[n // 2 : n // 2 + 1, :] for n in range(9)]
    re = {(a, a): q[a] for a in range(NB)}
    im = {}
    for n, (a, c) in enumerate(PAIRS):
        re[a, c] = re[c, a] = q[3 + n]
        im[a, c], im[c, a] = q[6 + n], -q[6 + n]

    def apply(xr, xi):
        ur, ui = [], []
        for a in range(NB):
            r, i = re[a, a] * xr[a], re[a, a] * xi[a]
            for c in range(NB):
                if c != a:
                    r = r + (re[a, c] * xr[c] - im[a, c] * xi[c])
                    i = i + (re[a, c] * xi[c] + im[a, c] * xr[c])
            ur.append(r)
            ui.append(i)
        return ur, ui

    def step(_, x):
        ur, ui = apply(x[:NB], x[NB:])
        norm = sum(r * r + i * i for r, i in zip(ur, ui))
        scale = lax.rsqrt(norm)
        return tuple(r * scale for r in ur) + tuple(i * scale for i in ui)

    one = jnp.ones_like(q[0])
    x = lax.fori_loop(0, ITERS, step, (one,) * NB + (one - one,) * NB)
    ur, ui = apply(x[:NB], x[NB:])
    energy = sum(x[a] * ur[a] + x[NB + a] * ui[a] for a in range(NB))
    factor = 1.0 / jnp.sqrt(jnp.maximum(energy, 0.25))
    return [v * factor for v in x], energy


def kernel(
    sizes, split_sizes, early, snap, wts_in, starts_in, bins_in, rec, tail, energy_out,
    wts, starts, bins, xbuf, lhs, rhs, spec, acc, g1, g1r, g2, g2r, coef, send, ahead, ahead_r,
    load_sem, small_sem, s1, r1, s2, r2, s3, r3, s4, r4,
):
    n_freq, n_pts, kf, n_var, n_time, n_local = sizes
    nx, nz, _ = split_sizes
    per_dev = kf // n_freq
    me_f = lax.axis_index("freq")
    n_oct, wide = n_freq // 8, 8
    cuts = [slice(128 * n, 128 * n + 128) for n in range(n_local // 128)]
    units = [(v, cut) for v in range(n_var) for cut in cuts]
    late, soon = units[: len(units) - early], units[len(units) - early :]

    def load(v):
        return pltpu.make_async_copy(snap.at[v], xbuf.at[v], load_sem.at[v])

    small = [
        pltpu.make_async_copy(source, target, small_sem.at[n])
        for n, (source, target) in enumerate(
            ((bins_in, bins), (starts_in, starts), (wts_in, wts))
        )
    ]
    for copy in small:
        copy.start()
    for v in range(n_var):
        load(v).start()

    barrier = pltpu.get_barrier_semaphore()
    near_group, far_group = groups_of(split_sizes)
    everyone = [p for pair in itertools.zip_longest(far_group[1], near_group[1]) for p in pair if p]
    for peer, _ in everyone:
        pl.semaphore_signal(barrier, inc=1, device_id=peer, device_id_type=MESH)

    acc[...] = jnp.zeros_like(acc)
    for copy in small:
        copy.wait()
    fill_tables(starts, bins, lhs, kf, n_time, per_dev)

    def centre(v, slot):
        x = xbuf[v]
        x = x - jnp.sum(x, axis=0, keepdims=True) * (1.0 / n_time)
        high, low = split(x)
        rhs[slot, 0:n_time, :] = high
        rhs[slot, n_time : 2 * n_time, :] = low
        rhs[slot, 2 * n_time : 3 * n_time, :] = high

    def gram(v):
        ws = [jnp.broadcast_to(wts[:, cut], (8, 128)) for cut in cuts]
        for octet in range(kf // 8):
            sums = [acc[pl.ds(n * HALF + octet * 8, 8), :] for n in range(9)]
            for w, cut in zip(ws, cuts):
                s = eight_bins(spec, kf, octet, v, cut)
                wt = [[w * part for part in one] for one in s]
                terms = [wt[a][0] * s[a][0] + wt[a][1] * s[a][1] for a in range(NB)]
                terms += [wt[a][0] * s[c][0] + wt[a][1] * s[c][1] for a, c in PAIRS]
                terms += [wt[a][0] * s[c][1] - wt[a][1] * s[c][0] for a, c in PAIRS]
                sums = [x + y for x, y in zip(sums, terms)]
            for n in range(9):
                acc[pl.ds(n * HALF + octet * 8, 8), :] = sums[n]

    def transform(v):
        spec[v] = jnp.dot(lhs[...], rhs[v], preferred_element_type=jnp.float32)

    for v in range(n_var):
        load(v).wait()
    centre(0, 0)
    for v in range(n_var):
        transform(v)
        if v + 1 < n_var:
            centre(v + 1, v + 1)
        if v:
            gram(v - 1)
    gram(n_var - 1)

    parts = acc[...]
    first = parts.astype(jnp.bfloat16)
    second, third = split(parts - first.astype(jnp.float32))
    by_lane = lax.dot_general(
        jnp.ones((8, 3 * 128), jnp.bfloat16),
        jnp.concatenate([first, second, third], axis=1),
        (((1,), (1,)), ((), ())),
        preferred_element_type=jnp.float32,
    )
    sublane = lax.broadcasted_iota(jnp.int32, (8, 128), 0)
    mine = jnp.zeros((8, 128), jnp.float32)
    for n in range(5):
        mine = jnp.where(sublane == n, by_lane[:, n * 128 : n * 128 + 128], mine)

    start_near, one_near, finish_near, drain_near = exchange(*near_group, g1, g1r, s1, r1)
    start_far, _, finish_far, drain_far = exchange(*far_group, g2, g2r, s2, r2)

    pitch = per_dev * early * 2 * NB

    def lead(dest, slot):
        return pltpu.make_async_remote_copy(
            src_ref=ahead.at[pl.ds(dest * pitch, pitch), :],
            dst_ref=ahead_r.at[pl.ds(slot * pitch, pitch), :],
            send_sem=s4,
            recv_sem=r4,
            device_id={"freq": dest},
            device_id_type=MESH,
        )

    def pack(octet, carry):
        for kk in range(per_dev):
            for n, (v, cut) in enumerate(soon):
                s = eight_bins(spec, kf, kk * n_oct + octet, v, cut)
                for b in range(NB):
                    for part in range(2):
                        at = octet * (8 * pitch) + ((kk * early + n) * NB + b) * 2 + part
                        ahead[pl.ds(at, wide, stride=pitch), :] = s[b][part]
        return carry

    if early:
        lax.fori_loop(0, n_oct, pack, 0)
        mine_rows = pl.ds(me_f * pitch, pitch)
        ahead_r[mine_rows, :] = ahead[mine_rows, :]

    x, z = me_f // nz, lax.rem(me_f, nz)

    def send_ahead(dz, steps):
        for dx in steps:
            dest = lax.rem(x + dx, nx) * nz + lax.rem(z + dz, nz)
            lead(dest, me_f).start()

    pl.semaphore_wait(barrier, len(everyone))
    start_near(mine[:5])
    order = sorted(range(1, nz), key=lambda d: min(d, nz - d))
    for dz in reversed(order):
        send_ahead(dz, (0,))
    others = range(1, nx)
    for dz in order[:2]:
        one_near(nz - dz)
        send_ahead(dz, others)
    for dz in order[2:]:
        one_near(nz - dz)
    near = finish_near()
    start_far(near)
    for dz in reversed(order[2:]):
        send_ahead(dz, others)
    send_ahead(0, others)
    total = finish_far()
    total = total / float(n_freq * n_pts * n_local * n_var)

    coefs, energy = leading(total)
    lane = lax.broadcasted_iota(jnp.int32, (1, 128), 1)
    for kk in range(per_dev):
        turned = pltpu.roll(energy, lax.rem(256 + kk - kk * n_freq - me_f, 128), 1)
        row = turned if kk == 0 else jnp.where(lane == kk, turned, row)
    energy_out[...] = row
    table = jnp.zeros((128, 128), jnp.float32)
    high = lax.broadcasted_iota(jnp.int32, (128, 128), 0)
    for n, c in enumerate(coefs):
        table = jnp.where(high == n, jnp.broadcast_to(c, (128, 128)), table)
    coef[...] = jnp.transpose(table)

    part_rows = len(late) * 2
    rows = per_dev * part_rows
    slot_rows = rows + 8

    def give(dest, slot):
        return pltpu.make_async_remote_copy(
            src_ref=send.at[pl.ds(dest * slot_rows, rows), :],
            dst_ref=rec.at[pl.ds(slot * rows, rows), :],
            send_sem=s3,
            recv_sem=r3,
            device_id={"freq": dest},
            device_id_type=MESH,
        )

    def spread(c):
        return [jnp.broadcast_to(c[:, n : n + 1], (8, 128)) for n in range(2 * NB)]

    def combine(c, s):
        re = sum(c[b] * s[b][0] - c[NB + b] * s[b][1] for b in range(NB))
        im = sum(c[b] * s[b][1] + c[NB + b] * s[b][0] for b in range(NB))
        return re, im

    def modes(i, carry):
        octet = lax.rem(me_f // 8 + 1 + i, n_oct)
        for kk in range(per_dev):
            c = spread(coef[pl.ds(kk * n_freq + octet * 8, 8), :])
            for n, (v, cut) in enumerate(late):
                s = eight_bins(spec, kf, kk * n_oct + octet, v, cut)
                for part, value in enumerate(combine(c, s)):
                    at = octet * (8 * slot_rows) + kk * part_rows + 2 * n + part
                    send[pl.ds(at, wide, stride=slot_rows), :] = value
        for d in range(wide):
            dest = octet * 8 + d

            @pl.when(dest != me_f)
            def _():
                give(dest, me_f).start()

            @pl.when(dest == me_f)
            def _():
                rec[pl.ds(me_f * rows, rows), :] = send[pl.ds(me_f * slot_rows, rows), :]

        return carry

    lax.fori_loop(0, n_oct, modes, 0)

    if early:
        theirs = ahead_r.at[pl.ds(0, (n_freq - 1) * pitch), :]
        pltpu.make_async_copy(theirs, theirs, r4).wait()
        for kk in range(per_dev):
            c = coef[pl.ds(kk * n_freq + me_f, 1), :]
            c = spread(jnp.broadcast_to(c, (8, 128)))
            for octet in range(n_oct):
                for n in range(early):
                    s = [
                        [
                            ahead_r[
                                pl.ds(
                                    octet * 8 * pitch + ((kk * early + n) * NB + b) * 2 + part,
                                    wide,
                                    stride=pitch,
                                ),
                                :,
                            ]
                            for part in range(2)
                        ]
                        for b in range(NB)
                    ]
                    for part, value in enumerate(combine([q for q in c], s)):
                        at = octet * 16 * per_dev * early + (kk * early + n) * 2 + part
                        tail[pl.ds(at, wide, stride=2 * per_dev * early), :] = value

    others = rec.at[pl.ds(0, (n_freq - 1) * rows), :]
    pltpu.make_async_copy(others, others, r3).wait()
    pltpu.make_async_copy(others, others, s3).wait()
    if early:
        pltpu.make_async_copy(theirs, theirs, s4).wait()
    drain_near()
    drain_far()


def write_out(sizes, early, rec, tail, row, modes, energy, held_energy, sems, sem):
    per_dev, n_var, tiles = sizes
    left = n_var * tiles - early
    copies = []

    def add(source, target):
        copies.append(pltpu.make_async_copy(source, target, sems.at[len(copies)]))

    for kk in range(per_dev):
        for v in range(n_var):
            held = modes.at[kk * n_var + v]
            if (v + 1) * tiles <= left:
                add(rec.at[:, kk, pl.ds(v * tiles, tiles)], held)
            elif v * tiles >= left:
                add(tail.at[:, pl.ds(kk * early + v * tiles - left, tiles)], held)
            else:
                cut = left - v * tiles
                add(rec.at[:, kk, pl.ds(v * tiles, cut)], held.at[:, pl.ds(0, cut)])
                add(
                    tail.at[:, pl.ds(kk * early, tiles - cut)],
                    held.at[:, pl.ds(cut, tiles - cut)],
                )
    held_energy[...] = row[0, :per_dev]
    last = pltpu.make_async_copy(held_energy, energy, sem)
    last.start()
    for copy in copies:
        copy.start()
    for copy in copies:
        copy.wait()
    last.wait()


def body(n_freq, n_pts, nz, snapshots, weights, starts, bins):
    n_time, n_var, n_local = snapshots.shape
    kf = bins.shape[0]
    per_dev = kf // n_freq
    tiles = n_local // 128
    early = 2
    rows = kf * (n_var * tiles - early) * 2
    ahead = max(kf * early * 2 * NB, 8)
    tail_rows = max(kf * early * 2, n_freq * 2)
    sizes = (n_freq, n_pts, kf, n_var, n_time, n_local)
    split_sizes = (n_freq // nz, nz, n_pts // 2)
    near, far = 2 * nz, split_sizes[0] * split_sizes[2]
    vmem, anywhere = (pl.BlockSpec(memory_space=m) for m in (pltpu.VMEM, pl.ANY))
    dma = pltpu.SemaphoreType.DMA
    rec, tail, energy = pl.pallas_call(
        functools.partial(kernel, sizes, split_sizes, early),
        out_shape=(
            pltpu.VMEM((rows, 128), jnp.float32),
            pltpu.VMEM((tail_rows, 128), jnp.float32),
            pltpu.VMEM((1, 128), jnp.float32),
        ),
        in_specs=[anywhere] * 4,
        out_specs=(vmem, vmem, vmem),
        scratch_shapes=[
            pltpu.VMEM((1, n_local), jnp.float32),
            pltpu.SMEM((NB,), jnp.int32),
            pltpu.VMEM((1, kf), jnp.int32),
            pltpu.VMEM((n_var, n_time, n_local), jnp.float32),
            pltpu.VMEM((2 * NB * kf, 3 * n_time), jnp.bfloat16),
            pltpu.VMEM((n_var, 3 * n_time, n_local), jnp.bfloat16),
            pltpu.VMEM((n_var, 2 * NB * kf, n_local), jnp.float32),
            pltpu.VMEM((10 * HALF, 128), jnp.float32),
            pltpu.VMEM((5, 128), jnp.float32),
            pltpu.VMEM((near, 5, 128), jnp.float32),
            pltpu.VMEM((5, 128), jnp.float32),
            pltpu.VMEM((far, 5, 128), jnp.float32),
            pltpu.VMEM((128, 128), jnp.float32),
            pltpu.VMEM((rows + 8 * n_freq, 128), jnp.float32),
            pltpu.VMEM((ahead, 128), jnp.float32),
            pltpu.VMEM((ahead, 128), jnp.float32),
            dma((n_var,)),
            dma((3,)),
        ]
        + [dma(()), dma((nz,)), dma(()), dma((1,))]
        + [dma(())] * 4,
        compiler_params=pltpu.CompilerParams(collective_id=0, has_side_effects=True),
    )(jnp.transpose(snapshots, (1, 0, 2)), weights.reshape(1, -1), starts, bins.reshape(1, -1))
    held = [
        pltpu.with_memory_space_constraint(value, pltpu.VMEM)
        for value in (
            rec.reshape(n_freq, per_dev, -1, 2, 128),
            tail.reshape(n_freq, -1, 2, 128),
            energy,
        )
    ]
    modes, energy = pl.pallas_call(
        functools.partial(write_out, (per_dev, n_var, tiles), early),
        out_shape=(
            jax.ShapeDtypeStruct((per_dev * n_var, n_freq, tiles, 2, 128), jnp.float32),
            jax.ShapeDtypeStruct((per_dev,), jnp.float32),
        ),
        in_specs=[vmem] * 3,
        out_specs=(anywhere, anywhere),
        scratch_shapes=[
            pltpu.VMEM((per_dev,), jnp.float32),
            dma((2 * per_dev * n_var,)),
            dma(()),
        ],
    )(*held)
    modes = modes.reshape(per_dev, n_var, n_freq * tiles, 2, 128)
    modes = jnp.transpose(modes, (0, 3, 1, 2, 4)).reshape(
        per_dev, 2, n_var, n_freq * n_local
    )
    return modes, energy


def solution(mesh):
    n_freq, n_pts = mesh.shape["freq"], mesh.shape["pts"]
    return jax.shard_map(
        functools.partial(body, n_freq, n_pts, LENGTH_Z),
        mesh=mesh,
        in_specs=(P(None, None, ("pts", "freq")), P(("pts", "freq")), P(), P()),
        out_specs=(P("freq", None, None, "pts"), P("freq")),
        check_vma=False,
    )
```

```python
import functools
import itertools
import math

import jax
import jax.numpy as jnp
from jax import lax
from jax.experimental import pallas as pl
from jax.experimental.pallas import tpu as pltpu
from jax.sharding import PartitionSpec as P

NFFT = 128
NB = 3
ITERS = 8
LENGTH_Z = 8
FAR_FIRST = (4, 3, 5, 2, 6, 1, 7, 0)
HALF = 64
PAIRS = ((0, 1), (0, 2), (1, 2))
MESH = pl.DeviceIdType.MESH


def half_angle(steps):
    h = steps.astype(jnp.float32) * (math.pi / NFFT)
    z = h * h
    s = jnp.float32(1.0 / math.factorial(13))
    for n in (11, 9, 7, 5, 3, 1):
        s = (1.0 if (n // 2) % 2 == 0 else -1.0) / math.factorial(n) + s * z
    c = jnp.float32(1.0 / math.factorial(12))
    for n in (10, 8, 6, 4, 2, 0):
        c = (1.0 if (n // 2) % 2 == 0 else -1.0) / math.factorial(n) + c * z
    return s * h, c


def split(value):
    high = value.astype(jnp.bfloat16)
    return high, (value - high.astype(jnp.float32)).astype(jnp.bfloat16)


def fill_tables(starts, bins, lhs, kf, n_time, per_dev):
    n_dev = kf // per_dev
    slot = lax.broadcasted_iota(jnp.int32, (kf, kf), 0)
    slot = lax.rem(slot, n_dev) * per_dev + slot // n_dev
    here = lax.broadcasted_iota(jnp.int32, (kf, kf), 1) == slot
    row = jnp.broadcast_to(bins[...].astype(jnp.float32), (kf, kf))
    column = jnp.sum(jnp.where(here, row, 0.0), axis=1, keepdims=True).astype(jnp.int32)
    lane = lax.broadcasted_iota(jnp.int32, (kf, NFFT), 1)
    time = lax.broadcasted_iota(jnp.int32, (1, n_time), 1)
    scale = 1.0 / math.sqrt(NFFT * 3 / 8)
    for block in range(NB):
        t = time - starts[block]
        sin_w, _ = half_angle(jnp.clip(64 - jnp.abs(t - 64), 0, 64))
        window = sin_w * sin_w * scale
        window = jnp.where((t >= 0) & (t < NFFT), window, 0.0)
        t = lane - starts[block]
        sin_h, cos_h = half_angle((((column * t) + 64) & (NFFT - 1)) - 64)
        for part, table in enumerate((1.0 - 2.0 * sin_h * sin_h, -2.0 * sin_h * cos_h)):
            rows = pl.ds((2 * block + part) * kf, kf)
            for n in range(n_time // NFFT):
                high, low = split(table * window[:, n * NFFT : (n + 1) * NFFT])
                for third, value in enumerate((high, high, low)):
                    at = third * n_time + n * NFFT
                    lhs[rows, at : at + NFFT] = value


def eight_bins(spec, kf, octet, v, cut):
    return [
        [spec[v, pl.ds((2 * b + part) * kf + octet * 8, 8), cut] for part in range(2)]
        for b in range(NB)
    ]


def exchange(slot, group, source, landed, sent, came):
    shared = sum(number == 0 for _, number in group)

    def wait(count, sem):
        held = landed.at[pl.ds(0, count)]
        pltpu.make_async_copy(held, held, sem).wait()

    def start(value):
        source[...] = value
        landed[slot] = value
        for peer, number in group:
            pltpu.make_async_remote_copy(
                src_ref=source,
                dst_ref=landed.at[slot],
                send_sem=sent,
                recv_sem=came.at[number],
                device_id=peer,
                device_id_type=MESH,
            ).start()

    def one(number):
        wait(1, came.at[number])

    def finish():
        wait(shared, came.at[0])
        total = landed[0]
        for n in range(1, len(group) + 1):
            total += landed[n]
        return total

    def drain():
        wait(len(group), sent)

    return start, one, finish, drain


def groups_of(sizes):
    nx, nz, ny = sizes
    f, p = lax.axis_index("freq"), lax.axis_index("pts")
    x, z, y, core = f // nz, lax.rem(f, nz), p // 2, lax.rem(p, 2)

    def far(d, n):
        return min(d, n - d)

    steps = [(i, j) for i in range(nx) for j in range(ny) if i or j]
    steps.sort(key=lambda s: -far(s[0], nx) - far(s[1], ny))
    plane = [
        ({"freq": lax.rem(x + i, nx) * nz + z, "pts": lax.rem(y + j, ny) * 2 + core}, 0)
        for i, j in steps
    ]
    steps = [(i, j) for i in range(nz) for j in range(2) if i or j]
    steps.sort(key=lambda s: -far(s[0], nz) - 0.5 * s[1])
    line = [
        ({"freq": x * nz + lax.rem(z + i, nz), "pts": y * 2 + lax.rem(core + j, 2)}, 0 if j else i)
        for i, j in steps
    ]
    return (z * 2 + core, line), (x * ny + y, plane)


def leading(total):
    other = pltpu.roll(total, HALF, 1)
    q = [(total if n % 2 == 0 else other)[n // 2 : n // 2 + 1, :] for n in range(9)]
    re = {(a, a): q[a] for a in range(NB)}
    im = {}
    for n, (a, c) in enumerate(PAIRS):
        re[a, c] = re[c, a] = q[3 + n]
        im[a, c], im[c, a] = q[6 + n], -q[6 + n]

    def apply(xr, xi):
        ur, ui = [], []
        for a in range(NB):
            r, i = re[a, a] * xr[a], re[a, a] * xi[a]
            for c in range(NB):
                if c != a:
                    r = r + (re[a, c] * xr[c] - im[a, c] * xi[c])
                    i = i + (re[a, c] * xi[c] + im[a, c] * xr[c])
            ur.append(r)
            ui.append(i)
        return ur, ui

    def step(_, x):
        ur, ui = apply(x[:NB], x[NB:])
        norm = sum(r * r + i * i for r, i in zip(ur, ui))
        scale = lax.rsqrt(norm)
        return tuple(r * scale for r in ur) + tuple(i * scale for i in ui)

    one = jnp.ones_like(q[0])
    x = lax.fori_loop(0, ITERS, step, (one,) * NB + (one - one,) * NB)
    ur, ui = apply(x[:NB], x[NB:])
    energy = sum(x[a] * ur[a] + x[NB + a] * ui[a] for a in range(NB))
    factor = 1.0 / jnp.sqrt(jnp.maximum(energy, 0.25))
    return [v * factor for v in x], energy


def kernel(
    sizes, split_sizes, early, snap, wts_in, starts_in, bins_in, rec, tail, energy_out,
    wts, starts, bins, xbuf, lhs, rhs, spec, acc, g1, g1r, g2, g2r, coef, send, ahead, ahead_r,
    load_sem, small_sem, s1, r1, s2, r2, s3, r3, s4, r4,
):
    n_freq, n_pts, kf, n_var, n_time, n_local = sizes
    nx, nz, _ = split_sizes
    per_dev = kf // n_freq
    me_f = lax.axis_index("freq")
    n_oct, wide = n_freq // 8, 8
    cuts = [slice(128 * n, 128 * n + 128) for n in range(n_local // 128)]
    units = [(v, cut) for v in range(n_var) for cut in cuts]
    late, soon = units[: len(units) - early], units[len(units) - early :]

    def load(v):
        return pltpu.make_async_copy(snap.at[v], xbuf.at[v], load_sem.at[v])

    small = [
        pltpu.make_async_copy(source, target, small_sem.at[n])
        for n, (source, target) in enumerate(
            ((bins_in, bins), (starts_in, starts), (wts_in, wts))
        )
    ]
    for copy in small:
        copy.start()
    for v in range(n_var):
        load(v).start()

    barrier = pltpu.get_barrier_semaphore()
    near_group, far_group = groups_of(split_sizes)
    everyone = [p for pair in itertools.zip_longest(far_group[1], near_group[1]) for p in pair if p]
    for peer, _ in everyone:
        pl.semaphore_signal(barrier, inc=1, device_id=peer, device_id_type=MESH)

    acc[...] = jnp.zeros_like(acc)
    for copy in small:
        copy.wait()
    fill_tables(starts, bins, lhs, kf, n_time, per_dev)

    def centre(v, slot):
        x = xbuf[v]
        x = x - jnp.sum(x, axis=0, keepdims=True) * (1.0 / n_time)
        high, low = split(x)
        rhs[slot, 0:n_time, :] = high
        rhs[slot, n_time : 2 * n_time, :] = low
        rhs[slot, 2 * n_time : 3 * n_time, :] = high

    def gram(v):
        ws = [jnp.broadcast_to(wts[:, cut], (8, 128)) for cut in cuts]
        for octet in range(kf // 8):
            sums = [acc[pl.ds(n * HALF + octet * 8, 8), :] for n in range(9)]
            for w, cut in zip(ws, cuts):
                s = eight_bins(spec, kf, octet, v, cut)
                wt = [[w * part for part in one] for one in s]
                terms = [wt[a][0] * s[a][0] + wt[a][1] * s[a][1] for a in range(NB)]
                terms += [wt[a][0] * s[c][0] + wt[a][1] * s[c][1] for a, c in PAIRS]
                terms += [wt[a][0] * s[c][1] - wt[a][1] * s[c][0] for a, c in PAIRS]
                sums = [x + y for x, y in zip(sums, terms)]
            for n in range(9):
                acc[pl.ds(n * HALF + octet * 8, 8), :] = sums[n]

    def transform(v):
        spec[v] = jnp.dot(lhs[...], rhs[v], preferred_element_type=jnp.float32)

    for v in range(n_var):
        load(v).wait()
    centre(0, 0)
    for v in range(n_var):
        transform(v)
        if v + 1 < n_var:
            centre(v + 1, v + 1)
        if v:
            gram(v - 1)
    gram(n_var - 1)

    parts = acc[...]
    first = parts.astype(jnp.bfloat16)
    second, third = split(parts - first.astype(jnp.float32))
    by_lane = lax.dot_general(
        jnp.ones((8, 3 * 128), jnp.bfloat16),
        jnp.concatenate([first, second, third], axis=1),
        (((1,), (1,)), ((), ())),
        preferred_element_type=jnp.float32,
    )
    sublane = lax.broadcasted_iota(jnp.int32, (8, 128), 0)
    mine = jnp.zeros((8, 128), jnp.float32)
    for n in range(5):
        mine = jnp.where(sublane == n, by_lane[:, n * 128 : n * 128 + 128], mine)

    start_near, one_near, finish_near, drain_near = exchange(*near_group, g1, g1r, s1, r1)
    start_far, _, finish_far, drain_far = exchange(*far_group, g2, g2r, s2, r2)

    pitch = per_dev * early * 2 * NB

    def lead(dest, slot):
        return pltpu.make_async_remote_copy(
            src_ref=ahead.at[pl.ds(dest * pitch, pitch), :],
            dst_ref=ahead_r.at[pl.ds(slot * pitch, pitch), :],
            send_sem=s4,
            recv_sem=r4,
            device_id={"freq": dest},
            device_id_type=MESH,
        )

    def pack(octet, carry):
        for kk in range(per_dev):
            for n, (v, cut) in enumerate(soon):
                s = eight_bins(spec, kf, kk * n_oct + octet, v, cut)
                for b in range(NB):
                    for part in range(2):
                        at = octet * (8 * pitch) + ((kk * early + n) * NB + b) * 2 + part
                        ahead[pl.ds(at, wide, stride=pitch), :] = s[b][part]
        return carry

    pl.semaphore_wait(barrier, len(everyone))
    start_near(mine[:5])
    if early:
        lax.fori_loop(0, n_oct, pack, 0)
        mine_rows = pl.ds(me_f * pitch, pitch)
        ahead_r[mine_rows, :] = ahead[mine_rows, :]

    x, z = me_f // nz, lax.rem(me_f, nz)

    def send_ahead(dz, steps):
        for dx in steps:
            dest = lax.rem(x + dx, nx) * nz + lax.rem(z + dz, nz)
            lead(dest, me_f).start()

    order = sorted(range(1, nz), key=lambda d: min(d, nz - d))
    for dz in reversed(order):
        send_ahead(dz, (0,))
    others = range(1, nx)
    for dz in order[:2]:
        one_near(nz - dz)
        send_ahead(dz, others)
    for dz in order[2:]:
        one_near(nz - dz)
    near = finish_near()
    start_far(near)
    for dz in reversed(order[2:]):
        send_ahead(dz, others)
    send_ahead(0, others)
    total = finish_far()
    total = total / float(n_freq * n_pts * n_local * n_var)

    coefs, energy = leading(total)
    lane = lax.broadcasted_iota(jnp.int32, (1, 128), 1)
    for kk in range(per_dev):
        turned = pltpu.roll(energy, lax.rem(256 + kk - kk * n_freq - me_f, 128), 1)
        row = turned if kk == 0 else jnp.where(lane == kk, turned, row)
    energy_out[...] = row
    table = jnp.zeros((128, 128), jnp.float32)
    high = lax.broadcasted_iota(jnp.int32, (128, 128), 0)
    for n, c in enumerate(coefs):
        table = jnp.where(high == n, jnp.broadcast_to(c, (128, 128)), table)
    coef[...] = jnp.transpose(table)

    part_rows = len(late) * 2
    rows = per_dev * part_rows
    slot_rows = rows + 8

    def give(dest, slot):
        return pltpu.make_async_remote_copy(
            src_ref=send.at[pl.ds(dest * slot_rows, rows), :],
            dst_ref=rec.at[pl.ds(slot * rows, rows), :],
            send_sem=s3,
            recv_sem=r3,
            device_id={"freq": dest},
            device_id_type=MESH,
        )

    def spread(c):
        return [jnp.broadcast_to(c[:, n : n + 1], (8, 128)) for n in range(2 * NB)]

    def combine(c, s):
        re = sum(c[b] * s[b][0] - c[NB + b] * s[b][1] for b in range(NB))
        im = sum(c[b] * s[b][1] + c[NB + b] * s[b][0] for b in range(NB))
        return re, im

    def modes(i, carry):
        octet = lax.rem(me_f // 8 + 1 + i, n_oct)
        for kk in range(per_dev):
            c = spread(coef[pl.ds(kk * n_freq + octet * 8, 8), :])
            for n, (v, cut) in enumerate(late):
                s = eight_bins(spec, kf, kk * n_oct + octet, v, cut)
                for part, value in enumerate(combine(c, s)):
                    at = octet * (8 * slot_rows) + kk * part_rows + 2 * n + part
                    send[pl.ds(at, wide, stride=slot_rows), :] = value
        for d in range(wide):
            dest = octet * 8 + d

            @pl.when(dest != me_f)
            def _():
                give(dest, me_f).start()

            @pl.when(dest == me_f)
            def _():
                rec[pl.ds(me_f * rows, rows), :] = send[pl.ds(me_f * slot_rows, rows), :]

        return carry

    lax.fori_loop(0, n_oct, modes, 0)

    if early:
        theirs = ahead_r.at[pl.ds(0, (n_freq - 1) * pitch), :]
        pltpu.make_async_copy(theirs, theirs, r4).wait()
        for kk in range(per_dev):
            c = coef[pl.ds(kk * n_freq + me_f, 1), :]
            c = spread(jnp.broadcast_to(c, (8, 128)))
            for octet in range(n_oct):
                for n in range(early):
                    s = [
                        [
                            ahead_r[
                                pl.ds(
                                    octet * 8 * pitch + ((kk * early + n) * NB + b) * 2 + part,
                                    wide,
                                    stride=pitch,
                                ),
                                :,
                            ]
                            for part in range(2)
                        ]
                        for b in range(NB)
                    ]
                    for part, value in enumerate(combine([q for q in c], s)):
                        at = octet * 16 * per_dev * early + (kk * early + n) * 2 + part
                        tail[pl.ds(at, wide, stride=2 * per_dev * early), :] = value

    others = rec.at[pl.ds(0, (n_freq - 1) * rows), :]
    pltpu.make_async_copy(others, others, r3).wait()
    pltpu.make_async_copy(others, others, s3).wait()
    if early:
        pltpu.make_async_copy(theirs, theirs, s4).wait()
    drain_near()
    drain_far()


def write_out(sizes, early, rec, tail, row, modes, energy, held_energy, sems, sem):
    per_dev, n_var, tiles = sizes
    left = n_var * tiles - early
    copies = []

    def add(source, target):
        copies.append(pltpu.make_async_copy(source, target, sems.at[len(copies)]))

    for kk in range(per_dev):
        for v in range(n_var):
            held = modes.at[kk * n_var + v]
            if (v + 1) * tiles <= left:
                add(rec.at[:, kk, pl.ds(v * tiles, tiles)], held)
            elif v * tiles >= left:
                add(tail.at[:, pl.ds(kk * early + v * tiles - left, tiles)], held)
            else:
                cut = left - v * tiles
                add(rec.at[:, kk, pl.ds(v * tiles, cut)], held.at[:, pl.ds(0, cut)])
                add(
                    tail.at[:, pl.ds(kk * early, tiles - cut)],
                    held.at[:, pl.ds(cut, tiles - cut)],
                )
    held_energy[...] = row[0, :per_dev]
    last = pltpu.make_async_copy(held_energy, energy, sem)
    last.start()
    for copy in copies:
        copy.start()
    for copy in copies:
        copy.wait()
    last.wait()


def body(n_freq, n_pts, nz, snapshots, weights, starts, bins):
    n_time, n_var, n_local = snapshots.shape
    kf = bins.shape[0]
    per_dev = kf // n_freq
    tiles = n_local // 128
    early = 2
    rows = kf * (n_var * tiles - early) * 2
    ahead = max(kf * early * 2 * NB, 8)
    tail_rows = max(kf * early * 2, n_freq * 2)
    sizes = (n_freq, n_pts, kf, n_var, n_time, n_local)
    split_sizes = (n_freq // nz, nz, n_pts // 2)
    near, far = 2 * nz, split_sizes[0] * split_sizes[2]
    vmem, anywhere = (pl.BlockSpec(memory_space=m) for m in (pltpu.VMEM, pl.ANY))
    dma = pltpu.SemaphoreType.DMA
    rec, tail, energy = pl.pallas_call(
        functools.partial(kernel, sizes, split_sizes, early),
        out_shape=(
            pltpu.VMEM((rows, 128), jnp.float32),
            pltpu.VMEM((tail_rows, 128), jnp.float32),
            pltpu.VMEM((1, 128), jnp.float32),
        ),
        in_specs=[anywhere] * 4,
        out_specs=(vmem, vmem, vmem),
        scratch_shapes=[
            pltpu.VMEM((1, n_local), jnp.float32),
            pltpu.SMEM((NB,), jnp.int32),
            pltpu.VMEM((1, kf), jnp.int32),
            pltpu.VMEM((n_var, n_time, n_local), jnp.float32),
            pltpu.VMEM((2 * NB * kf, 3 * n_time), jnp.bfloat16),
            pltpu.VMEM((n_var, 3 * n_time, n_local), jnp.bfloat16),
            pltpu.VMEM((n_var, 2 * NB * kf, n_local), jnp.float32),
            pltpu.VMEM((10 * HALF, 128), jnp.float32),
            pltpu.VMEM((5, 128), jnp.float32),
            pltpu.VMEM((near, 5, 128), jnp.float32),
            pltpu.VMEM((5, 128), jnp.float32),
            pltpu.VMEM((far, 5, 128), jnp.float32),
            pltpu.VMEM((128, 128), jnp.float32),
            pltpu.VMEM((rows + 8 * n_freq, 128), jnp.float32),
            pltpu.VMEM((ahead, 128), jnp.float32),
            pltpu.VMEM((ahead, 128), jnp.float32),
            dma((n_var,)),
            dma((3,)),
        ]
        + [dma(()), dma((nz,)), dma(()), dma((1,))]
        + [dma(())] * 4,
        compiler_params=pltpu.CompilerParams(collective_id=0, has_side_effects=True),
    )(jnp.transpose(snapshots, (1, 0, 2)), weights.reshape(1, -1), starts, bins.reshape(1, -1))
    held = [
        pltpu.with_memory_space_constraint(value, pltpu.VMEM)
        for value in (
            rec.reshape(n_freq, per_dev, -1, 2, 128),
            tail.reshape(n_freq, -1, 2, 128),
            energy,
        )
    ]
    modes, energy = pl.pallas_call(
        functools.partial(write_out, (per_dev, n_var, tiles), early),
        out_shape=(
            jax.ShapeDtypeStruct((per_dev * n_var, n_freq, tiles, 2, 128), jnp.float32),
            jax.ShapeDtypeStruct((per_dev,), jnp.float32),
        ),
        in_specs=[vmem] * 3,
        out_specs=(anywhere, anywhere),
        scratch_shapes=[
            pltpu.VMEM((per_dev,), jnp.float32),
            dma((2 * per_dev * n_var,)),
            dma(()),
        ],
    )(*held)
    modes = modes.reshape(per_dev, n_var, n_freq * tiles, 2, 128)
    modes = jnp.transpose(modes, (0, 3, 1, 2, 4)).reshape(
        per_dev, 2, n_var, n_freq * n_local
    )
    return modes, energy


def solution(mesh):
    n_freq, n_pts = mesh.shape["freq"], mesh.shape["pts"]
    return jax.shard_map(
        functools.partial(body, n_freq, n_pts, LENGTH_Z),
        mesh=mesh,
        in_specs=(P(None, None, ("pts", "freq")), P(("pts", "freq")), P(), P()),
        out_specs=(P("freq", None, None, "pts"), P("freq")),
        check_vma=False,
    )
```
